128 devices in a mesh: island: 8 (over x_lo, z), shard: 16 (over y, x_hi, core).
Axes of the slice: x: 4 (x_hi: 2, x_lo: 2; x = x_hi * 2 + x_lo), y: 4, z: 4, core: 2. Of those that a mesh axis runs over, the one named last changes fastest.
Arguments:
- weight_master: float32 [4096, 4096], P('island', 'shard'), may hold values from -6 to 6
- gain_master: float32 [4096], P(('shard', 'island')), may hold values from 0.5 to 1.5
- weight_moment: float32 [4096, 4096], P('island', 'shard'), may hold values from -0.3 to 0.3
- gain_moment: float32 [4096], P(('shard', 'island')), may hold values from -0.3 to 0.3
- attended: bfloat16 [8, 2, 1536, 4096], P('island', None, 'shard'), may hold values from -6 to 6
- stream: bfloat16 [8, 2, 1536, 4096], P('island', None, None, 'shard'), may hold values from -6 to 6
- targets: bfloat16 [8, 2, 1536, 4096], P('island', None, None, 'shard'), may hold values from -6 to 6
Outputs:
- weight_updated: float32 [4096, 4096], P('island', 'shard')
- gain_updated: float32 [4096], P(('shard', 'island'))
- weight_velocity: float32 [4096, 4096], P('island', 'shard')
- gain_velocity: float32 [4096], P(('shard', 'island'))
The draws below stay inside these ranges and needn't reach their ends.
All inputs are finite; a program needn't handle non-finite values.
Results may differ from the reference program's by a relative error of at most 0.0066.
Values may be sent and summed in bfloat16 or wider, within the bound.
No kernel may reach another device: no remote copies, remote signals or barrier semaphores. Data moves between devices by JAX's collectives and lax.ppermute only.
A program may use at most 192 MiB of HBM per device.

```python
import jax
import jax.numpy as jnp
from jax import lax

D = 4096
STEPS = 2
TOK = 1536
ISLANDS = 8
N_ISLAND = 8


def block_scale(own_key, shape, split, smallest, largest):
    loudness, own = 1.0, jax.random.fold_in(own_key, 6)
    for position, parts in split:
        heights = jnp.exp(jax.random.uniform(jax.random.fold_in(own, position), (parts,), jnp.float32, smallest / len(split), largest / len(split)))
        loudness = loudness * jnp.repeat(heights, shape[position] // parts).reshape([-1 if axis == position else 1 for axis in range(len(shape))])
    return loudness


def normal_values(own_key, extent, width, reach, shards=(), kind=jnp.bfloat16):
    result = width * jax.random.normal(own_key, extent, jnp.float32)
    if shards:
        result = result * block_scale(own_key, extent, shards, -0.22, 0.18)
    return jnp.clip(result, -reach, reach).astype(kind)


def setup_inputs(seed: int = 0) -> dict:
    arg_keys = jax.random.split(jax.random.key(seed), 8)
    return {
        "weight_master": normal_values(arg_keys[0], (D, D), 1.0, 6.0, ((0, 8), (1, 16)), jnp.float32),
        "gain_master": jnp.clip(1.0 + 0.1 * jax.random.normal(arg_keys[1], (D,), jnp.float32), 0.5, 1.5),
        "weight_moment": normal_values(arg_keys[2], (D, D), 0.05, 0.3, ((0, 8), (1, 16)), jnp.float32),
        "gain_moment": normal_values(arg_keys[3], (D,), 0.05, 0.3, ((0, 128),), jnp.float32),
        "attended": normal_values(arg_keys[4], (ISLANDS, STEPS, TOK, D), 1.0, 6.0, ((0, 8), (2, 16))),
        "stream": normal_values(arg_keys[5], (ISLANDS, STEPS, TOK, D), 1.0, 6.0, ((0, 8), (3, 16))),
        "targets": normal_values(arg_keys[6], (ISLANDS, STEPS, TOK, D), 1.0, 6.0, ((0, 8), (3, 16))),
    }


norm_epsilon = 1e-05
inner_rate = 0.05
beta_one = 0.9
beta_two = 0.95
adam_epsilon = 0.3
decay_rate = 0.1
outer_rate = 0.7
outer_momentum = 0.9

def optimizer_update(param, gradient, first, second, number, decay):
    first = beta_one * first + (1.0 - beta_one) * gradient
    second = beta_two * second + (1.0 - beta_two) * gradient * gradient
    first_hat = first / (1.0 - beta_one ** number)
    second_hat = second / (1.0 - beta_two ** number)
    param = param - inner_rate * (first_hat / (jnp.sqrt(second_hat) + adam_epsilon) + decay * param)
    return (param, first, second)

def rounded(value):
    return lax.optimization_barrier(value.astype(jnp.bfloat16)).astype(jnp.float32)

def island_window(weight_anchor, gain_anchor, attended_all, stream_all, goals_all):
    highest = lax.Precision.HIGHEST
    width_scale = D ** (-0.5)
    weight = weight_anchor
    gain = gain_anchor
    weight_first = jnp.zeros_like(weight)
    weight_second = jnp.zeros_like(weight)
    gain_first = jnp.zeros_like(gain)
    gain_second = jnp.zeros_like(gain)
    for inner_step in range(STEPS):
        number = inner_step + 1
        weight_low = weight.astype(jnp.bfloat16).astype(jnp.float32)
        rows_wide = attended_all[inner_step].astype(jnp.float32)
        projected = jnp.dot(rows_wide, weight_low, precision=highest) * width_scale
        residual = stream_all[inner_step].astype(jnp.float32) + projected
        inverse = lax.rsqrt(lax.optimization_barrier(jnp.mean(residual * residual, axis=1, keepdims=True)) + norm_epsilon)
        normed = residual * inverse * gain
        loss_grad = rounded(normed - goals_all[inner_step].astype(jnp.float32))
        scaled = loss_grad * gain
        slope = lax.optimization_barrier(jnp.sum(scaled * residual, axis=1, keepdims=True))
        residual_grad = rounded(inverse * scaled - residual * inverse * inverse * inverse * slope / D)
        weight_grad = jnp.dot(rows_wide.T, residual_grad, precision=highest) * width_scale
        gain_grad = lax.optimization_barrier(jnp.sum(loss_grad * residual * inverse, axis=0))
        weight, weight_first, weight_second = optimizer_update(weight, weight_grad, weight_first, weight_second, number, decay_rate)
        gain, gain_first, gain_second = optimizer_update(gain, gain_grad, gain_first, gain_second, number, 0.0)
    return (weight, gain)

def reference(weight_master, gain_master, weight_moment, gain_moment, attended, stream, targets):
    weight_anchor = rounded(weight_master)
    gain_anchor = rounded(gain_master)
    weight_total = jnp.zeros_like(weight_master)
    gain_total = jnp.zeros_like(gain_master)
    for island in range(N_ISLAND):
        weight_final, gain_final = island_window(weight_anchor, gain_anchor, attended[island], stream[island], targets[island])
        weight_total = weight_total + (weight_anchor - weight_final)
        gain_total = gain_total + (gain_anchor - gain_final)
    weight_pseudo = weight_total / N_ISLAND
    gain_pseudo = gain_total / N_ISLAND
    weight_velocity = outer_momentum * weight_moment + weight_pseudo
    gain_velocity = outer_momentum * gain_moment + gain_pseudo
    weight_updated = weight_master - outer_rate * (weight_pseudo + outer_momentum * weight_velocity)
    gain_updated = gain_master - outer_rate * (gain_pseudo + outer_momentum * gain_velocity)
    return (weight_updated, gain_updated, weight_velocity, gain_velocity)
```

```python
import jax
import jax.numpy as jnp
from jax import lax
from jax.experimental import pallas as pl
from jax.experimental.pallas import tpu as pltpu
from jax.sharding import Mesh
from jax.sharding import PartitionSpec as P


D = 4096
STEPS = 2
SHARD = ("y", "xh", "c")
SHARD_ISLAND = ("y", "xh", "c", "island")


norm_epsilon = 1e-05
inner_rate = 0.05
beta_one = 0.9
beta_two = 0.95
adam_epsilon = 0.3
decay_rate = 0.1
outer_rate = 0.7
outer_momentum = 0.9


def core_swap(value):
    return lax.ppermute(value, "c", [(0, 1), (1, 0)])


def x_swap(value):
    return lax.ppermute(value, "xh", [(0, 1), (1, 0)])


def y_hop(value, way):
    pairs = []
    for y in range(4):
        for c in range(2):
            to = (y + (way if c == 0 else -way)) % 4
            pairs.append((y * 2 + c, to * 2 + c))
    return lax.ppermute(value, ("y", "c"), pairs)


def copy_for_each(value, axis):
    copies = jnp.broadcast_to(value, (lax.axis_size(axis), *value.shape))
    return lax.all_to_all(copies, axis, split_axis=0, concat_axis=0, tiled=True)


def gathered_pieces(own):
    a = y_hop(own, 1)
    b = y_hop(own, -1)
    x = x_swap(own)
    a2 = y_hop(x, 1)
    b2 = y_hop(x, -1)
    f = y_hop(a, 1)
    f2 = y_hop(b2, -1)
    return (own, x, a, b, a2, b2, f, f2)


BLOCK = 96


def forward_kernel(*refs):
    pieces, (weight, weight_other, flow, residual, rows_out, rows, weights, came, loaded, left) = (
        refs[:8],
        refs[8:],
    )
    y, xh, c = lax.axis_index("y"), lax.axis_index("xh"), lax.axis_index("c")
    d = 1 - 2 * c
    before, after, across = (y + 4 - d) % 4, (y + 4 + d) % 4, (y + 2) % 4
    places = [
        (py * 2 + px) * BLOCK
        for py, px in (
            (y, xh), (y, 1 - xh), (before, xh), (after, xh),
            (before, 1 - xh), (after, 1 - xh), (across, xh), (across, 1 - xh),
        )
    ]
    wide = weight.shape[1]
    loads = [
        pltpu.make_async_copy(source, weights.at[half], loaded.at[half])
        for half, source in enumerate((weight, weight_other))
    ]
    takes = [
        pltpu.make_async_copy(source, rows.at[pl.ds(at * BLOCK, BLOCK)], came.at[at])
        for at, source in enumerate(pieces)
    ]
    gives = [
        pltpu.make_async_copy(
            rows.at[pl.ds(at * BLOCK, BLOCK)],
            rows_out.at[pl.ds(pl.multiple_of(places[at], BLOCK), BLOCK)],
            left.at[at],
        )
        for at in range(8)
    ]
    loads[0].start()
    for take in takes[:4]:
        take.start()
    loads[1].start()
    for take in takes[4:]:
        take.start()
    for group in range(2):
        members = range(group * 4, group * 4 + 4)
        for at in members:
            takes[at].wait()
            gives[at].start()
        for half in range(2):
            if group == 0:
                loads[half].wait()
            projected = jnp.dot(
                rows[group * 4 * BLOCK : (group + 1) * 4 * BLOCK, :],
                weights[half],
                preferred_element_type=jnp.float32,
            )
            columns = slice(half * wide, (half + 1) * wide)
            for place, at in enumerate(members):
                to = pl.ds(pl.multiple_of(places[at], BLOCK), BLOCK)
                residual[to, columns] = (
                    flow[to, columns].astype(jnp.float32)
                    + projected[place * BLOCK : (place + 1) * BLOCK] * D ** (-0.5)
                )
    for give in gives:
        give.wait()


def forward(pieces, weight, weight_other, flow):
    anywhere = pl.BlockSpec(memory_space=pl.ANY)
    inside = pl.BlockSpec(memory_space=pltpu.VMEM)
    tokens, features = flow.shape
    depth = weight.shape[0]
    return pl.pallas_call(
        forward_kernel,
        out_shape=(
            jax.ShapeDtypeStruct((tokens, features), jnp.float32),
            jax.ShapeDtypeStruct((tokens, depth), jnp.bfloat16),
        ),
        in_specs=[anywhere] * 10 + [inside],
        out_specs=(inside, anywhere),
        scratch_shapes=[
            pltpu.VMEM((tokens, depth), jnp.bfloat16),
            pltpu.VMEM((2, *weight.shape), jnp.bfloat16),
            pltpu.SemaphoreType.DMA((8,)),
            pltpu.SemaphoreType.DMA((2,)),
            pltpu.SemaphoreType.DMA((8,)),
        ],
        compiler_params=pltpu.CompilerParams(vmem_limit_bytes=24 * 1024 * 1024),
        cost_estimate=pl.CostEstimate(
            flops=2 * tokens * depth * features,
            bytes_accessed=4 * tokens * depth + 2 * depth * features,
            transcendentals=0,
        ),
        name="forward",
    )(*pieces, weight, weight_other, flow)


def first_update(param, gradient, decay):
    return param - inner_rate * (gradient / (jnp.abs(gradient) + adam_epsilon) + decay * param)


def second_update(param, before, gradient, decay):
    beside = (1.0 - beta_one) / (1.0 - beta_one**2)
    first_hat = (beta_one * beside) * before + beside * gradient
    beside = (1.0 - beta_two) / (1.0 - beta_two**2)
    second_hat = (beta_two * beside) * (before * before) + beside * (gradient * gradient)
    root = second_hat * lax.rsqrt(jnp.maximum(second_hat, 1e-37))
    return param - inner_rate * (first_hat / (root + adam_epsilon) + decay * param)


def per_device(weight_master, gain_master, weight_moment, gain_moment, attended, stream, targets):
    islands = lax.axis_size("island")
    width_scale = D ** (-0.5)
    c = lax.axis_index("c")
    wide = weight_master.shape[1]

    pieces = [gathered_pieces(attended[0][step]) for step in range(STEPS)]

    anchor_low = copy_for_each(weight_master.astype(jnp.bfloat16), "island")
    anchor_low = anchor_low.reshape(D, wide)
    gain_low = copy_for_each(gain_master.astype(jnp.bfloat16), "island").reshape(wide)

    def token_half(value):
        blocks = value[0].reshape(STEPS, 8, 2, 96, wide)
        mine = lax.dynamic_index_in_dim(blocks, c, axis=2, keepdims=False)
        theirs = lax.dynamic_index_in_dim(blocks, 1 - c, axis=2, keepdims=False)
        both = jnp.concatenate([mine, core_swap(theirs)], axis=-1)
        return both.reshape(STEPS, 768, 2 * wide)

    stream_half = token_half(stream)
    target_half = token_half(targets)

    weight_anchor = anchor_low.astype(jnp.float32)
    weight_low = anchor_low
    gain_anchor = gain_low.astype(jnp.float32)
    gain = jnp.concatenate([gain_anchor, core_swap(gain_low).astype(jnp.float32)])
    weight = weight_anchor
    for step in range(STEPS):
        weight_other = core_swap(weight_low)
        residual, rows = forward(pieces[step], weight_low, weight_other, stream_half[step])
        goal = target_half[step].astype(jnp.float32)
        scaled = residual * gain
        sums = [
            jnp.sum(residual * residual, axis=1),
            jnp.sum(scaled * scaled, axis=1),
            jnp.sum(goal * scaled, axis=1),
        ]
        sums = jnp.concatenate(sums).reshape(1, -1)
        totals = copy_for_each(sums, ("y", "xh"))
        totals = jnp.sum(totals, axis=0).reshape(3, -1)
        inverse = lax.rsqrt(totals[0] / D + norm_epsilon)
        slope = (inverse * totals[1] - totals[2])[:, None]
        inverse = inverse[:, None]
        normed = residual * inverse * gain
        loss_grad = lax.optimization_barrier((normed - goal).astype(jnp.bfloat16))
        loss_grad = loss_grad.astype(jnp.float32)
        residual_grad = (
            inverse * (loss_grad * gain) - residual * inverse * inverse * inverse * slope / D
        ).astype(jnp.bfloat16)
        gain_grad = jnp.sum(loss_grad * residual * inverse, axis=0)

        def over_tokens(columns):
            return jnp.einsum(
                "td,tf->df", rows, residual_grad[:, columns], preferred_element_type=jnp.float32
            )

        other = over_tokens(slice(wide, None)).astype(jnp.bfloat16)
        other = core_swap(other)
        mine = over_tokens(slice(0, wide))
        weight_grad = (mine + other.astype(jnp.float32)) * width_scale
        gain_other = core_swap(gain_grad)
        gain_grad = gain_grad + jnp.concatenate([gain_other[wide:], gain_other[:wide]])
        if step == 0:
            weight = first_update(weight, weight_grad, decay_rate)
            gain = first_update(gain, gain_grad, 0.0)
            weight_low = weight.astype(jnp.bfloat16)
            weight, weight_before, gain_before, weight_low = lax.optimization_barrier(
                (weight, weight_grad, gain_grad, weight_low)
            )
        else:
            weight = second_update(weight, weight_before, weight_grad, decay_rate)
            gain = second_update(gain, gain_before, gain_grad, 0.0)

    def sent_and_summed(value):
        blocks = value.reshape(islands, value.shape[0] // islands, *value.shape[1:])
        arrived = lax.all_to_all(blocks, "island", split_axis=0, concat_axis=0, tiled=True)
        return arrived.astype(jnp.float32).sum(axis=0)

    weight_pseudo = sent_and_summed((weight_anchor - weight).astype(jnp.bfloat16)) / islands
    gain_pseudo = sent_and_summed((gain_anchor - gain[:wide]).astype(jnp.bfloat16)) / islands
    weight_velocity = outer_momentum * weight_moment + weight_pseudo
    gain_velocity = outer_momentum * gain_moment + gain_pseudo
    weight_updated = weight_master - outer_rate * (weight_pseudo + outer_momentum * weight_velocity)
    gain_updated = gain_master - outer_rate * (gain_pseudo + outer_momentum * gain_velocity)
    return (weight_updated, gain_updated, weight_velocity, gain_velocity)


def solution(mesh):
    torus = Mesh(
        mesh.devices.reshape(mesh.shape["island"], 4, 2, 2), ("island", "y", "xh", "c")
    )
    return jax.shard_map(
        per_device,
        mesh=torus,
        in_specs=(
            P("island", SHARD),
            P(SHARD_ISLAND),
            P("island", SHARD),
            P(SHARD_ISLAND),
            P("island", None, SHARD, None),
            P("island", None, None, SHARD),
            P("island", None, None, SHARD),
        ),
        out_specs=(P("island", SHARD), P(SHARD_ISLAND), P("island", SHARD), P(SHARD_ISLAND)),
        check_vma=False,
    )
```

```python
import jax
import jax.numpy as jnp
from jax import lax
from jax.experimental import pallas as pl
from jax.experimental.pallas import tpu as pltpu
from jax.sharding import Mesh
from jax.sharding import PartitionSpec as P


D = 4096
STEPS = 2
SHARD = ("y", "xh", "c")
SHARD_ISLAND = ("y", "xh", "c", "island")


norm_epsilon = 1e-05
inner_rate = 0.05
beta_one = 0.9
beta_two = 0.95
adam_epsilon = 0.3
decay_rate = 0.1
outer_rate = 0.7
outer_momentum = 0.9


def core_swap(value):
    return lax.ppermute(value, "c", [(0, 1), (1, 0)])


def x_swap(value):
    return lax.ppermute(value, "xh", [(0, 1), (1, 0)])


def y_hop(value, way):
    pairs = []
    for y in range(4):
        for c in range(2):
            to = (y + (way if c == 0 else -way)) % 4
            pairs.append((y * 2 + c, to * 2 + c))
    return lax.ppermute(value, ("y", "c"), pairs)


def copy_for_each(value, axis):
    copies = jnp.broadcast_to(value, (lax.axis_size(axis), *value.shape))
    return lax.all_to_all(copies, axis, split_axis=0, concat_axis=0, tiled=True)


def gathered_pieces(own):
    a = y_hop(own, 1)
    b = y_hop(own, -1)
    x = x_swap(own)
    a2 = y_hop(x, 1)
    b2 = y_hop(x, -1)
    f = y_hop(a, 1)
    f2 = y_hop(b2, -1)
    return (own, x, a, b, a2, b2, f, f2)


BLOCK = 96


def forward_kernel(*refs):
    pieces, (weight, weight_other, flow, residual, rows_out, rows, weights, came, loaded, left) = (
        refs[:8],
        refs[8:],
    )
    y, xh, c = lax.axis_index("y"), lax.axis_index("xh"), lax.axis_index("c")
    d = 1 - 2 * c
    before, after, across = (y + 4 - d) % 4, (y + 4 + d) % 4, (y + 2) % 4
    places = [
        (py * 2 + px) * BLOCK
        for py, px in (
            (y, xh), (y, 1 - xh), (before, xh), (after, xh),
            (before, 1 - xh), (after, 1 - xh), (across, xh), (across, 1 - xh),
        )
    ]
    wide = weight.shape[2]
    loads = [
        pltpu.make_async_copy(
            source.at[:, pl.ds(0, weights.shape[2])], weights.at[half], loaded.at[half]
        )
        for half, source in enumerate((weight, weight_other))
    ]
    takes = [
        pltpu.make_async_copy(source, rows.at[pl.ds(at * BLOCK, BLOCK)], came.at[at])
        for at, source in enumerate(pieces)
    ]
    gives = [
        pltpu.make_async_copy(
            rows.at[pl.ds(at * BLOCK, BLOCK)],
            rows_out.at[pl.ds(pl.multiple_of(places[at], BLOCK), BLOCK)],
            left.at[at],
        )
        for at in range(8)
    ]
    loads[0].start()
    for take in takes[:4]:
        take.start()
    loads[1].start()
    for take in takes[4:]:
        take.start()
    for group in range(2):
        members = range(group * 4, group * 4 + 4)
        for at in members:
            takes[at].wait()
            gives[at].start()
        for half in range(2):
            if group == 0:
                loads[half].wait()
            projected = jnp.dot(
                rows[group * 4 * BLOCK : (group + 1) * 4 * BLOCK, :],
                weights[half].reshape(D, wide),
                preferred_element_type=jnp.float32,
            )
            columns = slice(half * wide, (half + 1) * wide)
            for place, at in enumerate(members):
                to = pl.ds(pl.multiple_of(places[at], BLOCK), BLOCK)
                residual[to, columns] = (
                    flow[to, columns].astype(jnp.float32)
                    + projected[place * BLOCK : (place + 1) * BLOCK] * D ** (-0.5)
                )
    for give in gives:
        give.wait()


def forward(pieces, weight, weight_other, flow):
    anywhere = pl.BlockSpec(memory_space=pl.ANY)
    inside = pl.BlockSpec(memory_space=pltpu.VMEM)
    tokens, features = flow.shape
    depth = D
    islands, _, wide = weight.shape
    return pl.pallas_call(
        forward_kernel,
        out_shape=(
            jax.ShapeDtypeStruct((tokens, features), jnp.float32),
            jax.ShapeDtypeStruct((tokens, depth), jnp.bfloat16),
        ),
        in_specs=[anywhere] * 10 + [inside],
        out_specs=(inside, pl.BlockSpec(memory_space=pltpu.HBM)),
        scratch_shapes=[
            pltpu.VMEM((tokens, depth), jnp.bfloat16),
            pltpu.VMEM((2, islands, depth // islands, wide), jnp.bfloat16),
            pltpu.SemaphoreType.DMA((8,)),
            pltpu.SemaphoreType.DMA((2,)),
            pltpu.SemaphoreType.DMA((8,)),
        ],
        compiler_params=pltpu.CompilerParams(vmem_limit_bytes=24 * 1024 * 1024),
        cost_estimate=pl.CostEstimate(
            flops=2 * tokens * depth * features,
            bytes_accessed=4 * tokens * depth + 2 * depth * features,
            transcendentals=0,
        ),
        name="forward",
    )(*pieces, weight, weight_other, flow)


def first_update(param, gradient, decay):
    return param - inner_rate * (gradient / (jnp.abs(gradient) + adam_epsilon) + decay * param)


def second_update(param, before, gradient, decay):
    beside = (1.0 - beta_one) / (1.0 - beta_one**2)
    first_hat = (beta_one * beside) * before + beside * gradient
    beside = (1.0 - beta_two) / (1.0 - beta_two**2)
    second_hat = (beta_two * beside) * (before * before) + beside * (gradient * gradient)
    root = second_hat * lax.rsqrt(jnp.maximum(second_hat, 1e-37))
    return param - inner_rate * (first_hat / (root + adam_epsilon) + decay * param)


def per_device(weight_master, gain_master, weight_moment, gain_moment, attended, stream, targets):
    islands = lax.axis_size("island")
    width_scale = D ** (-0.5)
    c = lax.axis_index("c")
    wide = weight_master.shape[1]

    pieces = [gathered_pieces(attended[0][step]) for step in range(STEPS)]

    def with_gain(weight_rows, gain_rows):
        filled = [(0, 0)] * (gain_rows.ndim - 1) + [(0, 15), (0, wide - gain_rows.shape[-1])]
        return jnp.concatenate([weight_rows, jnp.pad(gain_rows[..., None, :], filled)], axis=-2)

    owned, share = weight_master.shape[0], gain_master.shape[0]
    packed = with_gain(weight_master.astype(jnp.bfloat16), gain_master.astype(jnp.bfloat16))
    packed = copy_for_each(packed, "island")
    packed_other = core_swap(packed)
    anchor_low = packed[:, :owned].reshape(D, wide)
    gain_anchor = packed[:, owned, :share].reshape(wide).astype(jnp.float32)
    gain_other = packed_other[:, owned, :share].reshape(wide).astype(jnp.float32)

    def token_half(value):
        blocks = value[0].reshape(STEPS, 8, 2, 96, wide)
        mine = lax.dynamic_index_in_dim(blocks, c, axis=2, keepdims=False)
        theirs = lax.dynamic_index_in_dim(blocks, 1 - c, axis=2, keepdims=False)
        both = jnp.concatenate([mine, core_swap(theirs)], axis=-1)
        return both.reshape(STEPS, 768, 2 * wide)

    stream_half = token_half(stream)
    target_half = token_half(targets)

    weight_anchor = anchor_low.astype(jnp.float32)
    gain = jnp.concatenate([gain_anchor, gain_other])
    weight = weight_anchor
    for step in range(STEPS):
        if step == 0:
            held, held_other = packed, packed_other
        else:
            held = weight_low.reshape(islands, owned, wide)
            held_other = core_swap(held)
        residual, rows = forward(pieces[step], held, held_other, stream_half[step])
        goal = target_half[step].astype(jnp.float32)
        scaled = residual * gain
        sums = [
            jnp.sum(residual * residual, axis=1),
            jnp.sum(scaled * scaled, axis=1),
            jnp.sum(goal * scaled, axis=1),
        ]
        sums = jnp.concatenate(sums).reshape(1, -1)
        totals = copy_for_each(sums, ("y", "xh"))
        totals = jnp.sum(totals, axis=0).reshape(3, -1)
        inverse = lax.rsqrt(totals[0] / D + norm_epsilon)
        slope = (inverse * totals[1] - totals[2])[:, None]
        inverse = inverse[:, None]
        normed = residual * inverse * gain
        loss_grad = lax.optimization_barrier((normed - goal).astype(jnp.bfloat16))
        loss_grad = loss_grad.astype(jnp.float32)
        residual_grad = (
            inverse * (loss_grad * gain) - residual * inverse * inverse * inverse * slope / D
        ).astype(jnp.bfloat16)
        gain_grad = jnp.sum(loss_grad * residual * inverse, axis=0)

        def over_tokens(columns):
            return jnp.einsum(
                "td,tf->df", rows, residual_grad[:, columns], preferred_element_type=jnp.float32
            )

        other = over_tokens(slice(wide, None)).astype(jnp.bfloat16)
        other = core_swap(other)
        mine = lax.optimization_barrier(over_tokens(slice(0, wide)))
        weight_grad = (mine + other.astype(jnp.float32)) * width_scale
        gain_other = core_swap(gain_grad)
        gain_grad = gain_grad + jnp.concatenate([gain_other[wide:], gain_other[:wide]])
        if step == 0:
            weight = first_update(weight, weight_grad, decay_rate)
            gain = first_update(gain, gain_grad, 0.0)
            weight_low = weight.astype(jnp.bfloat16)
            weight, weight_before, gain_before, weight_low = lax.optimization_barrier(
                (weight, weight_grad, gain_grad, weight_low)
            )
        else:
            weight = second_update(weight, weight_before, weight_grad, decay_rate)
            gain = second_update(gain, gain_before, gain_grad, 0.0)

    sent = with_gain(
        (weight_anchor - weight).astype(jnp.bfloat16).reshape(islands, owned, wide),
        (gain_anchor - gain[:wide]).astype(jnp.bfloat16).reshape(islands, share),
    )
    arrived = lax.all_to_all(sent, "island", split_axis=0, concat_axis=0, tiled=True)
    pseudo = arrived.astype(jnp.float32).sum(axis=0) / islands
    weight_pseudo, gain_pseudo = pseudo[:owned], pseudo[owned, :share]
    weight_velocity = outer_momentum * weight_moment + weight_pseudo
    gain_velocity = outer_momentum * gain_moment + gain_pseudo
    weight_updated = weight_master - outer_rate * (weight_pseudo + outer_momentum * weight_velocity)
    gain_updated = gain_master - outer_rate * (gain_pseudo + outer_momentum * gain_velocity)
    return (weight_updated, gain_updated, weight_velocity, gain_velocity)


def solution(mesh):
    torus = Mesh(
        mesh.devices.reshape(mesh.shape["island"], 4, 2, 2), ("island", "y", "xh", "c")
    )
    return jax.shard_map(
        per_device,
        mesh=torus,
        in_specs=(
            P("island", SHARD),
            P(SHARD_ISLAND),
            P("island", SHARD),
            P(SHARD_ISLAND),
            P("island", None, SHARD, None),
            P("island", None, None, SHARD),
            P("island", None, None, SHARD),
        ),
        out_specs=(P("island", SHARD), P(SHARD_ISLAND), P("island", SHARD), P(SHARD_ISLAND)),
        check_vma=False,
    )
```

```python
import jax
import jax.numpy as jnp
from jax import lax
from jax.experimental import pallas as pl
from jax.experimental.pallas import tpu as pltpu
from jax.sharding import Mesh
from jax.sharding import PartitionSpec as P


D = 4096
STEPS = 2
SHARD = ("y", "xh", "c")
ISLAND = ("xl", "z")
SHARD_ISLAND = ("y", "xh", "c", "xl", "z")


norm_epsilon = 1e-05
inner_rate = 0.05
beta_one = 0.9
beta_two = 0.95
adam_epsilon = 0.3
decay_rate = 0.1
outer_rate = 0.7
outer_momentum = 0.9


def core_swap(value):
    return lax.ppermute(value, "c", [(0, 1), (1, 0)])


def x_swap(value):
    return lax.ppermute(value, "xh", [(0, 1), (1, 0)])


def y_hop(value, way):
    pairs = []
    for y in range(4):
        for c in range(2):
            to = (y + (way if c == 0 else -way)) % 4
            pairs.append((y * 2 + c, to * 2 + c))
    return lax.ppermute(value, ("y", "c"), pairs)


def copy_for_each(value, axis):
    copies = jnp.broadcast_to(value, (lax.axis_size(axis), *value.shape))
    return lax.all_to_all(copies, axis, split_axis=0, concat_axis=0, tiled=True)


def gathered_pieces(own):
    a = y_hop(own, 1)
    b = y_hop(own, -1)
    x = x_swap(own)
    a2 = y_hop(x, 1)
    b2 = y_hop(x, -1)
    f = y_hop(a, 1)
    f2 = y_hop(b2, -1)
    return (own, x, a, b, a2, b2, f, f2)


BLOCK = 96
VMEM_LIMIT = 44 * 1024 * 1024


LETTERS = "oxabcefg"
SOON = ("oxabf", "oxabce")
LATE = ("ceg", "fg")


def forward_kernel(letters, pieces, weight, weight_other, flow, residual_out, rows_out, rows, weights, made, came, loaded, left, sent):
    y, xh, c = lax.axis_index("y"), lax.axis_index("xh"), lax.axis_index("c")
    d = 1 - 2 * c
    before, after, across = (y + 4 - d) % 4, (y + 4 + d) % 4, (y + 2) % 4
    blocks = (
        (y, xh), (y, 1 - xh), (before, xh), (after, xh),
        (before, 1 - xh), (after, 1 - xh), (across, xh), (across, 1 - xh),
    )
    places = []
    for letter in letters:
        py, px = blocks[LETTERS.index(letter)]
        places.append(pl.ds(pl.multiple_of((py * 2 + px) * BLOCK, BLOCK), BLOCK))
    own = [pl.ds(at * BLOCK, BLOCK) for at in range(len(letters))]
    islands, owned, wide = weights.shape[1:]

    def loads_of(half, source):
        if len(source.shape) == 3:
            return [pltpu.make_async_copy(source, weights.at[half], loaded.at[half, 0])]
        return [
            pltpu.make_async_copy(
                source.at[:, xl, pl.ds(0, owned)],
                weights.at[half, pl.ds(xl * (islands // 2), islands // 2)],
                loaded.at[half, xl],
            )
            for xl in range(2)
        ]

    loads = [loads_of(0, weight), loads_of(1, weight_other)]
    takes = [
        pltpu.make_async_copy(source, rows.at[at], came.at[i])
        for i, (at, source) in enumerate(zip(own, pieces))
    ]
    gives = [
        pltpu.make_async_copy(rows.at[at], rows_out.at[to], left.at[i])
        for i, (at, to) in enumerate(zip(own, places))
    ]
    sends = [
        pltpu.make_async_copy(made.at[at], residual_out.at[to], sent.at[i])
        for i, (at, to) in enumerate(zip(own, places))
    ]
    for copy in (*loads[0], *takes, *loads[1]):
        copy.start()
    for take, give in zip(takes, gives):
        take.wait()
        give.start()
    for half in range(2):
        for load in loads[half]:
            load.wait()
        projected = jnp.dot(
            rows[...],
            weights[half].reshape(islands * owned, wide),
            preferred_element_type=jnp.float32,
        )
        columns = slice(half * wide, (half + 1) * wide)
        for at, (mine, to) in enumerate(zip(own, places)):
            made[mine, columns] = (
                flow[to, columns].astype(jnp.float32)
                + projected[at * BLOCK : (at + 1) * BLOCK] * D ** (-0.5)
            )
    for send in sends:
        send.start()
    for copy in (*gives, *sends):
        copy.wait()


def forward(letters, pieces, weight, weight_other, flow, earlier=()):
    anywhere = pl.BlockSpec(memory_space=pl.ANY)
    inside = pl.BlockSpec(memory_space=pltpu.VMEM)
    count = len(letters)
    tokens, features = flow.shape
    islands, owned, wide = 8, D // 8, features // 2

    def kernel(*refs):
        rest = refs[count : count + 3] + refs[count + 3 + len(earlier) :]
        forward_kernel(letters, refs[:count], *rest)

    return pl.pallas_call(
        kernel,
        out_shape=(
            jax.ShapeDtypeStruct((tokens, features), jnp.float32),
            jax.ShapeDtypeStruct((tokens, D), jnp.bfloat16),
        ),
        in_specs=[anywhere] * (count + 2) + [inside] + [anywhere] * len(earlier),
        out_specs=(anywhere, anywhere),
        scratch_shapes=[
            pltpu.VMEM((count * BLOCK, D), jnp.bfloat16),
            pltpu.VMEM((2, islands, owned, wide), jnp.bfloat16),
            pltpu.VMEM((count * BLOCK, features), jnp.float32),
            pltpu.SemaphoreType.DMA((count,)),
            pltpu.SemaphoreType.DMA((2, 2)),
            pltpu.SemaphoreType.DMA((count,)),
            pltpu.SemaphoreType.DMA((count,)),
        ],
        input_output_aliases={count + 3 + i: i for i in range(len(earlier))},
        compiler_params=pltpu.CompilerParams(vmem_limit_bytes=VMEM_LIMIT),
        cost_estimate=pl.CostEstimate(
            flops=2 * count * BLOCK * D * features,
            bytes_accessed=4 * count * BLOCK * D + 2 * D * features,
            transcendentals=0,
        ),
        name="forward",
    )(*pieces, weight, weight_other, flow, *earlier)


def first_update(param, gradient, decay):
    return param - inner_rate * (gradient / (jnp.abs(gradient) + adam_epsilon) + decay * param)


def second_change(anchor, change, before, gradient, decay):
    beside = (1.0 - beta_one) / (1.0 - beta_one**2)
    first_hat = (beta_one * beside) * before + beside * gradient
    beside = (1.0 - beta_two) / (1.0 - beta_two**2)
    second_hat = (beta_two * beside) * (before * before) + beside * (gradient * gradient)
    root = second_hat * lax.rsqrt(jnp.maximum(second_hat, 1e-37))
    param = anchor - change
    return change + inner_rate * (first_hat / (root + adam_epsilon) + decay * param)


def per_device(weight_master, gain_master, weight_moment, gain_moment, attended, stream, targets):
    islands = lax.axis_size(ISLAND)
    width_scale = D ** (-0.5)
    c = lax.axis_index("c")
    wide = weight_master.shape[1]

    pieces = [gathered_pieces(attended[0][step]) for step in range(STEPS)]

    def with_gain(weight_rows, gain_rows):
        filled = [(0, 0)] * (gain_rows.ndim - 1) + [(0, 15), (0, wide - gain_rows.shape[-1])]
        return jnp.concatenate([weight_rows, jnp.pad(gain_rows[..., None, :], filled)], axis=-2)

    owned, share = weight_master.shape[0], gain_master.shape[0]
    packed = with_gain(weight_master.astype(jnp.bfloat16), gain_master.astype(jnp.bfloat16))
    beyond = lax.ppermute(packed, "xl", [(0, 1), (1, 0)])
    low = lax.axis_index("xl") == 0
    pair = jnp.stack([jnp.where(low, packed, beyond), jnp.where(low, beyond, packed)])
    packed = copy_for_each(pair, "z")
    packed_other = core_swap(packed)

    def in_island_order(value):
        return jnp.swapaxes(value, 0, 1)

    slabs = [packed[z, xl, :owned] for xl in range(2) for z in range(4)]
    anchor_low = lax.optimization_barrier(jnp.concatenate(slabs, axis=0))
    gain_anchor = in_island_order(packed[:, :, owned, :share]).reshape(wide).astype(jnp.float32)
    gain_other = in_island_order(packed_other[:, :, owned, :share]).reshape(wide)
    gain_other = gain_other.astype(jnp.float32)

    def token_half(value):
        blocks = value[0].reshape(STEPS, 8, 2, 96, wide)
        mine = lax.dynamic_index_in_dim(blocks, c, axis=2, keepdims=False)
        theirs = lax.dynamic_index_in_dim(blocks, 1 - c, axis=2, keepdims=False)
        both = jnp.concatenate([mine, core_swap(theirs)], axis=-1)
        return both.reshape(STEPS, 768, 2 * wide)

    stream_half = token_half(stream)
    target_half = token_half(targets)

    weight_anchor = anchor_low.astype(jnp.float32)
    gain = jnp.concatenate([gain_anchor, gain_other])
    for step in range(STEPS):
        if step == 0:
            held, held_other = packed, packed_other
        else:
            held = weight_low.reshape(islands, owned, wide)
            held_other = core_swap(held)
        earlier = ()
        for letters in (SOON[step], LATE[step]):
            some = [pieces[step][LETTERS.index(letter)] for letter in letters]
            earlier = forward(letters, some, held, held_other, stream_half[step], earlier)
        residual, rows = earlier
        goal = target_half[step].astype(jnp.float32)
        scaled = residual * gain
        sums = [
            jnp.sum(residual * residual, axis=1),
            jnp.sum(scaled * scaled, axis=1),
            jnp.sum(goal * scaled, axis=1),
        ]
        sums = jnp.concatenate(sums).reshape(1, -1)
        totals = copy_for_each(sums, ("y", "xh"))
        totals = jnp.sum(totals, axis=0).reshape(3, -1)
        inverse = lax.rsqrt(totals[0] / D + norm_epsilon)
        slope = (inverse * totals[1] - totals[2])[:, None]
        inverse = inverse[:, None]
        normed = residual * inverse * gain
        loss_grad = lax.optimization_barrier((normed - goal).astype(jnp.bfloat16))
        loss_grad = loss_grad.astype(jnp.float32)
        residual_grad = (
            inverse * (loss_grad * gain) - residual * inverse * inverse * inverse * slope / D
        ).astype(jnp.bfloat16)
        gain_grad = jnp.sum(loss_grad * residual * inverse, axis=0)

        def over_tokens(columns):
            return jnp.einsum(
                "td,tf->df", rows, residual_grad[:, columns], preferred_element_type=jnp.float32
            )

        other = over_tokens(slice(wide, None)).astype(jnp.bfloat16)
        other = core_swap(other)
        mine = lax.optimization_barrier(over_tokens(slice(0, wide)))
        weight_grad = (mine + other.astype(jnp.float32)) * width_scale
        gain_other = core_swap(gain_grad)
        gain_grad = gain_grad + jnp.concatenate([gain_other[wide:], gain_other[:wide]])
        if step == 0:
            weight_low = first_update(weight_anchor, weight_grad, decay_rate)
            weight_change = (weight_anchor - weight_low).astype(jnp.bfloat16)
            weight_before = weight_grad.astype(jnp.bfloat16)
            weight_low = weight_low.astype(jnp.bfloat16)
            gain_first = gain
            gain_before, gain = gain_grad, first_update(gain, gain_grad, 0.0)
            weight_change, weight_before, weight_low = lax.optimization_barrier(
                (weight_change, weight_before, weight_low)
            )
        else:
            weight_change = second_change(
                weight_anchor,
                weight_change.astype(jnp.float32),
                weight_before.astype(jnp.float32),
                weight_grad,
                decay_rate,
            )
            gain_change = second_change(gain_first, gain_first - gain, gain_before, gain_grad, 0.0)

    sent = with_gain(
        weight_change.astype(jnp.bfloat16).reshape(islands, owned, wide),
        gain_change[:wide].astype(jnp.bfloat16).reshape(islands, share),
    )
    arrived = lax.all_to_all(sent, ISLAND, split_axis=0, concat_axis=0, tiled=True)
    pseudo = arrived.astype(jnp.float32).sum(axis=0) / islands
    weight_pseudo, gain_pseudo = pseudo[:owned], pseudo[owned, :share]
    weight_velocity = outer_momentum * weight_moment + weight_pseudo
    gain_velocity = outer_momentum * gain_moment + gain_pseudo
    weight_updated = weight_master - outer_rate * (weight_pseudo + outer_momentum * weight_velocity)
    gain_updated = gain_master - outer_rate * (gain_pseudo + outer_momentum * gain_velocity)
    return (weight_updated, gain_updated, weight_velocity, gain_velocity)


def solution(mesh):
    torus = Mesh(mesh.devices.reshape(2, 4, 4, 2, 2), (*ISLAND, *SHARD))
    return jax.shard_map(
        per_device,
        mesh=torus,
        in_specs=(
            P(ISLAND, SHARD),
            P(SHARD_ISLAND),
            P(ISLAND, SHARD),
            P(SHARD_ISLAND),
            P(ISLAND, None, SHARD, None),
            P(ISLAND, None, None, SHARD),
            P(ISLAND, None, None, SHARD),
        ),
        out_specs=(P(ISLAND, SHARD), P(SHARD_ISLAND), P(ISLAND, SHARD), P(SHARD_ISLAND)),
        check_vma=False,
    )
```

```python
import jax
import jax.numpy as jnp
from jax import lax
from jax.experimental import pallas as pl
from jax.experimental.pallas import tpu as pltpu
from jax.sharding import Mesh
from jax.sharding import PartitionSpec as P


D = 4096
STEPS = 2
SHARD = ("y", "xh", "c")
ISLAND = ("xl", "z")
SHARD_ISLAND = ("y", "xh", "c", "xl", "z")


norm_epsilon = 1e-05
inner_rate = 0.05
beta_one = 0.9
beta_two = 0.95
adam_epsilon = 0.3
decay_rate = 0.1
outer_rate = 0.7
outer_momentum = 0.9


def core_swap(value):
    return lax.ppermute(value, "c", [(0, 1), (1, 0)])


def x_swap(value):
    return lax.ppermute(value, "xh", [(0, 1), (1, 0)])


def y_hop(value, way):
    pairs = []
    for y in range(4):
        for c in range(2):
            to = (y + (way if c == 0 else -way)) % 4
            pairs.append((y * 2 + c, to * 2 + c))
    return lax.ppermute(value, ("y", "c"), pairs)


def copy_for_each(value, axis):
    copies = jnp.broadcast_to(value, (lax.axis_size(axis), *value.shape))
    return lax.all_to_all(copies, axis, split_axis=0, concat_axis=0, tiled=True)


def gathered_pieces(own):
    a = y_hop(own, 1)
    b = y_hop(own, -1)
    x = x_swap(own)
    a2 = y_hop(x, 1)
    b2 = y_hop(x, -1)
    f = y_hop(a, 1)
    f2 = y_hop(b2, -1)
    return (own, x, a, b, a2, b2, f, f2)


BLOCK = 96
VMEM_LIMIT = 46 * 1024 * 1024


LETTERS = "oxabcefg"
SOON = ("oxabf", "oxabce")
LATE = ("ceg", "fg")


def forward_kernel(letters, pieces, weight, weight_other, flow, residual_out, rows_out, rows, made, came, left, sent):
    y, xh, c = lax.axis_index("y"), lax.axis_index("xh"), lax.axis_index("c")
    d = 1 - 2 * c
    before, after, across = (y + 4 - d) % 4, (y + 4 + d) % 4, (y + 2) % 4
    blocks = (
        (y, xh), (y, 1 - xh), (before, xh), (after, xh),
        (before, 1 - xh), (after, 1 - xh), (across, xh), (across, 1 - xh),
    )
    places = []
    for letter in letters:
        py, px = blocks[LETTERS.index(letter)]
        places.append(pl.ds(pl.multiple_of((py * 2 + px) * BLOCK, BLOCK), BLOCK))
    own = [pl.ds(at * BLOCK, BLOCK) for at in range(len(letters))]
    owned, wide = D // 8, flow.shape[1] // 2

    takes = [
        pltpu.make_async_copy(source, rows.at[at], came.at[i])
        for i, (at, source) in enumerate(zip(own, pieces))
    ]
    gives = [
        pltpu.make_async_copy(rows.at[at], rows_out.at[to], left.at[i])
        for i, (at, to) in enumerate(zip(own, places))
    ]
    sends = [
        pltpu.make_async_copy(made.at[at], residual_out.at[to], sent.at[i])
        for i, (at, to) in enumerate(zip(own, places))
    ]
    for take in takes:
        take.start()
    for take, give in zip(takes, gives):
        take.wait()
        give.start()
    for half, source in enumerate((weight, weight_other)):
        projected = 0.0
        for slab in range(8):
            if len(source.shape) == 3:
                part = source[slab]
            else:
                part = source[slab % 4, slab // 4, :owned]
            projected += jnp.dot(
                rows[:, slab * owned : (slab + 1) * owned],
                part,
                preferred_element_type=jnp.float32,
            )
        columns = slice(half * wide, (half + 1) * wide)
        for at, (mine, to) in enumerate(zip(own, places)):
            made[mine, columns] = (
                flow[to, columns].astype(jnp.float32)
                + projected[at * BLOCK : (at + 1) * BLOCK] * D ** (-0.5)
            )
    for send in sends:
        send.start()
    for copy in (*gives, *sends):
        copy.wait()


def forward(letters, pieces, weight, weight_other, flow, earlier=()):
    anywhere = pl.BlockSpec(memory_space=pl.ANY)
    inside = pl.BlockSpec(memory_space=pltpu.VMEM)
    count = len(letters)
    tokens, features = flow.shape

    def kernel(*refs):
        rest = refs[count : count + 3] + refs[count + 3 + len(earlier) :]
        forward_kernel(letters, refs[:count], *rest)

    return pl.pallas_call(
        kernel,
        out_shape=(
            jax.ShapeDtypeStruct((tokens, features), jnp.float32),
            jax.ShapeDtypeStruct((tokens, D), jnp.bfloat16),
        ),
        in_specs=[anywhere] * count + [inside] * 3 + [anywhere] * len(earlier),
        out_specs=(anywhere, anywhere),
        scratch_shapes=[
            pltpu.VMEM((count * BLOCK, D), jnp.bfloat16),
            pltpu.VMEM((count * BLOCK, features), jnp.float32),
            pltpu.SemaphoreType.DMA((count,)),
            pltpu.SemaphoreType.DMA((count,)),
            pltpu.SemaphoreType.DMA((count,)),
        ],
        input_output_aliases={count + 3 + i: i for i in range(len(earlier))},
        compiler_params=pltpu.CompilerParams(vmem_limit_bytes=VMEM_LIMIT),
        cost_estimate=pl.CostEstimate(
            flops=2 * count * BLOCK * D * features,
            bytes_accessed=4 * count * BLOCK * D + 2 * D * features,
            transcendentals=0,
        ),
        name="forward",
    )(*pieces, weight, weight_other, flow, *earlier)


def first_update(param, gradient, decay):
    return param - inner_rate * (gradient / (jnp.abs(gradient) + adam_epsilon) + decay * param)


def second_change(anchor, change, before, gradient, decay):
    beside = (1.0 - beta_one) / (1.0 - beta_one**2)
    first_hat = (beta_one * beside) * before + beside * gradient
    beside = (1.0 - beta_two) / (1.0 - beta_two**2)
    second_hat = (beta_two * beside) * (before * before) + beside * (gradient * gradient)
    root = second_hat * lax.rsqrt(jnp.maximum(second_hat, 1e-37))
    param = anchor - change
    return change + inner_rate * (first_hat / (root + adam_epsilon) + decay * param)


def per_device(weight_master, gain_master, weight_moment, gain_moment, attended, stream, targets):
    islands = lax.axis_size(ISLAND)
    width_scale = D ** (-0.5)
    c = lax.axis_index("c")
    wide = weight_master.shape[1]

    pieces = [gathered_pieces(attended[0][step]) for step in range(STEPS)]

    def with_gain(weight_rows, gain_rows):
        filled = [(0, 0)] * (gain_rows.ndim - 1) + [(0, 15), (0, wide - gain_rows.shape[-1])]
        return jnp.concatenate([weight_rows, jnp.pad(gain_rows[..., None, :], filled)], axis=-2)

    owned, share = weight_master.shape[0], gain_master.shape[0]
    packed = with_gain(weight_master.astype(jnp.bfloat16), gain_master.astype(jnp.bfloat16))
    beyond = lax.ppermute(packed, "xl", [(0, 1), (1, 0)])
    low = lax.axis_index("xl") == 0
    pair = jnp.stack([jnp.where(low, packed, beyond), jnp.where(low, beyond, packed)])
    packed = copy_for_each(pair, "z")
    packed_other = core_swap(packed)

    def in_island_order(value):
        return jnp.swapaxes(value, 0, 1)

    slabs = [packed[z, xl, :owned] for xl in range(2) for z in range(4)]
    anchor_low = lax.optimization_barrier(jnp.concatenate(slabs, axis=0))
    gain_anchor = in_island_order(packed[:, :, owned, :share]).reshape(wide).astype(jnp.float32)
    gain_other = in_island_order(packed_other[:, :, owned, :share]).reshape(wide)
    gain_other = gain_other.astype(jnp.float32)

    def token_half(value):
        blocks = value[0].reshape(STEPS, 8, 2, 96, wide)
        mine = lax.dynamic_index_in_dim(blocks, c, axis=2, keepdims=False)
        theirs = lax.dynamic_index_in_dim(blocks, 1 - c, axis=2, keepdims=False)
        both = jnp.concatenate([mine, core_swap(theirs)], axis=-1)
        return both.reshape(STEPS, 768, 2 * wide)

    stream_half = token_half(stream)
    target_half = token_half(targets)

    weight_anchor = anchor_low.astype(jnp.float32)
    gain = jnp.concatenate([gain_anchor, gain_other])
    for step in range(STEPS):
        if step == 0:
            held, held_other = packed, packed_other
        else:
            held = weight_low.reshape(islands, owned, wide)
            held_other = core_swap(held)
        earlier = ()
        for letters in (SOON[step], LATE[step]):
            some = [pieces[step][LETTERS.index(letter)] for letter in letters]
            earlier = forward(letters, some, held, held_other, stream_half[step], earlier)
        residual, rows = earlier
        goal = target_half[step].astype(jnp.float32)
        scaled = residual * gain
        sums = [
            jnp.sum(residual * residual, axis=1),
            jnp.sum(scaled * scaled, axis=1),
            jnp.sum(goal * scaled, axis=1),
        ]
        sums = jnp.concatenate(sums).reshape(1, -1)
        totals = copy_for_each(sums, ("y", "xh"))
        totals = jnp.sum(totals, axis=0).reshape(3, -1)
        inverse = lax.rsqrt(totals[0] / D + norm_epsilon)
        slope = (inverse * totals[1] - totals[2])[:, None]
        inverse = inverse[:, None]
        normed = residual * inverse * gain
        loss_grad = lax.optimization_barrier((normed - goal).astype(jnp.bfloat16))
        loss_grad = loss_grad.astype(jnp.float32)
        residual_grad = (
            inverse * (loss_grad * gain) - residual * inverse * inverse * inverse * slope / D
        ).astype(jnp.bfloat16)
        gain_grad = jnp.sum(loss_grad * residual * inverse, axis=0)

        def over_tokens(columns):
            return jnp.einsum(
                "td,tf->df", rows, residual_grad[:, columns], preferred_element_type=jnp.float32
            )

        other = over_tokens(slice(wide, None)).astype(jnp.bfloat16)
        other = core_swap(other)
        mine = over_tokens(slice(0, wide))
        if step == 0:
            mine = lax.optimization_barrier(mine)
        weight_grad = (mine + other.astype(jnp.float32)) * width_scale
        gain_other = core_swap(gain_grad)
        gain_grad = gain_grad + jnp.concatenate([gain_other[wide:], gain_other[:wide]])
        if step == 0:
            weight_low = first_update(weight_anchor, weight_grad, decay_rate)
            weight_change = (weight_anchor - weight_low).astype(jnp.bfloat16)
            weight_before = weight_grad.astype(jnp.bfloat16)
            weight_low = weight_low.astype(jnp.bfloat16)
            gain_first = gain
            gain_before, gain = gain_grad, first_update(gain, gain_grad, 0.0)
            weight_change, weight_before, weight_low = lax.optimization_barrier(
                (weight_change, weight_before, weight_low)
            )
        else:
            weight_change = second_change(
                weight_anchor,
                weight_change.astype(jnp.float32),
                weight_before.astype(jnp.float32),
                weight_grad,
                decay_rate,
            )
            gain_change = second_change(gain_first, gain_first - gain, gain_before, gain_grad, 0.0)

    sent = with_gain(
        weight_change.astype(jnp.bfloat16).reshape(islands, owned, wide),
        gain_change[:wide].astype(jnp.bfloat16).reshape(islands, share),
    )
    arrived = lax.all_to_all(sent, ISLAND, split_axis=0, concat_axis=0, tiled=True)
    pseudo = arrived.astype(jnp.float32).sum(axis=0) / islands
    weight_pseudo, gain_pseudo = pseudo[:owned], pseudo[owned, :share]
    weight_velocity = outer_momentum * weight_moment + weight_pseudo
    gain_velocity = outer_momentum * gain_moment + gain_pseudo
    weight_updated = weight_master - outer_rate * (weight_pseudo + outer_momentum * weight_velocity)
    gain_updated = gain_master - outer_rate * (gain_pseudo + outer_momentum * gain_velocity)
    return (weight_updated, gain_updated, weight_velocity, gain_velocity)


def solution(mesh):
    torus = Mesh(mesh.devices.reshape(2, 4, 4, 2, 2), (*ISLAND, *SHARD))
    return jax.shard_map(
        per_device,
        mesh=torus,
        in_specs=(
            P(ISLAND, SHARD),
            P(SHARD_ISLAND),
            P(ISLAND, SHARD),
            P(SHARD_ISLAND),
            P(ISLAND, None, SHARD, None),
            P(ISLAND, None, None, SHARD),
            P(ISLAND, None, None, SHARD),
        ),
        out_specs=(P(ISLAND, SHARD), P(SHARD_ISLAND), P(ISLAND, SHARD), P(SHARD_ISLAND)),
        check_vma=False,
    )
```

```python
import jax
import jax.numpy as jnp
from jax import lax
from jax.experimental import pallas as pl
from jax.experimental.pallas import tpu as pltpu
from jax.sharding import Mesh
from jax.sharding import PartitionSpec as P


D = 4096
STEPS = 2
SHARD = ("y", "xh", "c")
ISLAND = ("xl", "z")
SHARD_ISLAND = ("y", "xh", "c", "xl", "z")


norm_epsilon = 1e-05
inner_rate = 0.05
beta_one = 0.9
beta_two = 0.95
adam_epsilon = 0.3
decay_rate = 0.1
outer_rate = 0.7
outer_momentum = 0.9


def core_swap(value):
    return lax.ppermute(value, "c", [(0, 1), (1, 0)])


def x_swap(value):
    return lax.ppermute(value, "xh", [(0, 1), (1, 0)])


def y_hop(value, way):
    pairs = []
    for y in range(4):
        for c in range(2):
            to = (y + (way if c == 0 else -way)) % 4
            pairs.append((y * 2 + c, to * 2 + c))
    return lax.ppermute(value, ("y", "c"), pairs)


def copy_for_each(value, axis):
    copies = jnp.broadcast_to(value, (lax.axis_size(axis), *value.shape))
    return lax.all_to_all(copies, axis, split_axis=0, concat_axis=0, tiled=True)


def gathered_pieces(own):
    a = y_hop(own, 1)
    b = y_hop(own, -1)
    x = x_swap(own)
    a2 = y_hop(x, 1)
    b2 = y_hop(x, -1)
    f = y_hop(a, 1)
    f2 = y_hop(b2, -1)
    return (own, x, a, b, a2, b2, f, f2)


BLOCK = 96
VMEM_LIMIT = 40 * 1024 * 1024


LETTERS = "oxabcefg"


def forward_kernel(letters, pieces, weight, weight_other, flow, residual_out, rows_out, rows, weights, held, made, came, loaded, streamed, left, sent):
    y, xh, c = lax.axis_index("y"), lax.axis_index("xh"), lax.axis_index("c")
    d = 1 - 2 * c
    before, after, across = (y + 4 - d) % 4, (y + 4 + d) % 4, (y + 2) % 4
    blocks = (
        (y, xh), (y, 1 - xh), (before, xh), (after, xh),
        (before, 1 - xh), (after, 1 - xh), (across, xh), (across, 1 - xh),
    )
    places = []
    for letter in letters:
        py, px = blocks[LETTERS.index(letter)]
        places.append(pl.ds(pl.multiple_of((py * 2 + px) * BLOCK, BLOCK), BLOCK))
    own = [pl.ds(at * BLOCK, BLOCK) for at in range(len(letters))]
    owned, wide = D // 8, flow.shape[1] // 2

    loads = [
        pltpu.make_async_copy(
            source.at[:, pl.ds(0, owned)], weights.at[half], loaded.at[half]
        )
        for half, source in enumerate((weight, weight_other))
    ]
    flows = [
        pltpu.make_async_copy(flow.at[to], held.at[at], streamed.at[i])
        for i, (at, to) in enumerate(zip(own, places))
    ]
    takes = [
        pltpu.make_async_copy(source, rows.at[at], came.at[i])
        for i, (at, source) in enumerate(zip(own, pieces))
    ]
    gives = [
        pltpu.make_async_copy(rows.at[at], rows_out.at[to], left.at[i])
        for i, (at, to) in enumerate(zip(own, places))
    ]
    sends = [
        pltpu.make_async_copy(made.at[at], residual_out.at[to], sent.at[i])
        for i, (at, to) in enumerate(zip(own, places))
    ]
    for copy in (loads[0], *takes, *flows, loads[1]):
        copy.start()
    for take, give in zip(takes, gives):
        take.wait()
        give.start()
    for load in flows:
        load.wait()
    for half in range(2):
        loads[half].wait()
        projected = jnp.dot(
            rows[...], weights[half].reshape(D, wide), preferred_element_type=jnp.float32
        )
        columns = slice(half * wide, (half + 1) * wide)
        made[:, columns] = held[:, columns].astype(jnp.float32) + projected * D ** (-0.5)
    for send in sends:
        send.start()
    for copy in (*gives, *sends):
        copy.wait()


def forward(letters, pieces, weight, weight_other, flow, earlier=()):
    anywhere = pl.BlockSpec(memory_space=pl.ANY)
    count = len(letters)
    tokens, features = flow.shape

    def kernel(*refs):
        rest = refs[count : count + 3] + refs[count + 3 + len(earlier) :]
        forward_kernel(letters, refs[:count], *rest)

    return pl.pallas_call(
        kernel,
        out_shape=(
            jax.ShapeDtypeStruct((tokens, features), jnp.float32),
            jax.ShapeDtypeStruct((tokens, D), jnp.bfloat16),
        ),
        in_specs=[anywhere] * (count + 3 + len(earlier)),
        out_specs=(anywhere, anywhere),
        scratch_shapes=[
            pltpu.VMEM((count * BLOCK, D), jnp.bfloat16),
            pltpu.VMEM((2, 8, D // 8, features // 2), jnp.bfloat16),
            pltpu.VMEM((count * BLOCK, features), jnp.bfloat16),
            pltpu.VMEM((count * BLOCK, features), jnp.float32),
            pltpu.SemaphoreType.DMA((count,)),
            pltpu.SemaphoreType.DMA((2,)),
            pltpu.SemaphoreType.DMA((count,)),
            pltpu.SemaphoreType.DMA((count,)),
            pltpu.SemaphoreType.DMA((count,)),
        ],
        input_output_aliases={count + 3 + i: i for i in range(len(earlier))},
        compiler_params=pltpu.CompilerParams(vmem_limit_bytes=VMEM_LIMIT),
        cost_estimate=pl.CostEstimate(
            flops=2 * count * BLOCK * D * features,
            bytes_accessed=4 * count * BLOCK * D + 2 * D * features,
            transcendentals=0,
        ),
        name="forward",
    )(*pieces, weight, weight_other, flow, *earlier)


def first_update(param, gradient, decay):
    return param - inner_rate * (gradient / (jnp.abs(gradient) + adam_epsilon) + decay * param)


def second_change(anchor, change, before, gradient, decay):
    beside = (1.0 - beta_one) / (1.0 - beta_one**2)
    first_hat = (beta_one * beside) * before + beside * gradient
    beside = (1.0 - beta_two) / (1.0 - beta_two**2)
    second_hat = (beta_two * beside) * (before * before) + beside * (gradient * gradient)
    root = second_hat * lax.rsqrt(jnp.maximum(second_hat, 1e-37))
    param = anchor - change
    return change + inner_rate * (first_hat / (root + adam_epsilon) + decay * param)


def per_device(weight_master, gain_master, weight_moment, gain_moment, attended, stream, targets):
    islands = lax.axis_size(ISLAND)
    width_scale = D ** (-0.5)
    c = lax.axis_index("c")
    wide = weight_master.shape[1]

    pieces = [gathered_pieces(attended[0][step]) for step in range(STEPS)]

    def with_gain(weight_rows, gain_rows):
        filled = [(0, 0)] * (gain_rows.ndim - 1) + [(0, 15), (0, wide - gain_rows.shape[-1])]
        return jnp.concatenate([weight_rows, jnp.pad(gain_rows[..., None, :], filled)], axis=-2)

    owned, share = weight_master.shape[0], gain_master.shape[0]
    packed = with_gain(weight_master.astype(jnp.bfloat16), gain_master.astype(jnp.bfloat16))
    packed = copy_for_each(packed, ISLAND)
    packed_other = core_swap(packed)
    anchor_low = packed[:, :owned].reshape(D, wide)
    gain_anchor = packed[:, owned, :share].reshape(wide).astype(jnp.float32)
    gain_other = packed_other[:, owned, :share].reshape(wide).astype(jnp.float32)

    def token_half(value):
        blocks = value[0].reshape(STEPS, 8, 2, 96, wide)
        mine = lax.dynamic_index_in_dim(blocks, c, axis=2, keepdims=False)
        theirs = lax.dynamic_index_in_dim(blocks, 1 - c, axis=2, keepdims=False)
        both = jnp.concatenate([mine, core_swap(theirs)], axis=-1)
        return both.reshape(STEPS, 768, 2 * wide)

    stream_half = token_half(stream)
    target_half = token_half(targets)

    weight_anchor = anchor_low.astype(jnp.float32)
    gain = jnp.concatenate([gain_anchor, gain_other])
    for step in range(STEPS):
        if step == 0:
            held, held_other = packed, packed_other
        else:
            held = weight_low.reshape(islands, owned, wide)
            held_other = core_swap(held)
        residual, rows = forward(LETTERS, pieces[step], held, held_other, stream_half[step])
        goal = target_half[step].astype(jnp.float32)
        scaled = residual * gain
        sums = [
            jnp.sum(residual * residual, axis=1),
            jnp.sum(scaled * scaled, axis=1),
            jnp.sum(goal * scaled, axis=1),
        ]
        sums = jnp.concatenate(sums).reshape(1, -1)
        totals = copy_for_each(sums, ("y", "xh"))
        totals = jnp.sum(totals, axis=0).reshape(3, -1)
        inverse = lax.rsqrt(totals[0] / D + norm_epsilon)
        slope = (inverse * totals[1] - totals[2])[:, None]
        inverse = inverse[:, None]
        normed = residual * inverse * gain
        loss_grad = lax.optimization_barrier((normed - goal).astype(jnp.bfloat16))
        loss_grad = loss_grad.astype(jnp.float32)
        residual_grad = (
            inverse * (loss_grad * gain) - residual * inverse * inverse * inverse * slope / D
        ).astype(jnp.bfloat16)
        gain_grad = jnp.sum(loss_grad * residual * inverse, axis=0)

        def over_tokens(columns):
            return jnp.einsum(
                "td,tf->df", rows, residual_grad[:, columns], preferred_element_type=jnp.float32
            )

        other = over_tokens(slice(wide, None)).astype(jnp.bfloat16)
        other = core_swap(other)
        mine = lax.optimization_barrier(over_tokens(slice(0, wide)).astype(jnp.bfloat16))
        weight_grad = (mine.astype(jnp.float32) + other.astype(jnp.float32)) * width_scale
        gain_other = core_swap(gain_grad)
        gain_grad = gain_grad + jnp.concatenate([gain_other[wide:], gain_other[:wide]])
        if step == 0:
            weight_low = first_update(weight_anchor, weight_grad, decay_rate)
            weight_change = (weight_anchor - weight_low).astype(jnp.bfloat16)
            weight_before = weight_grad.astype(jnp.bfloat16)
            weight_low = weight_low.astype(jnp.bfloat16)
            gain_first = gain
            gain_before, gain = gain_grad, first_update(gain, gain_grad, 0.0)
            weight_change, weight_before, weight_low = lax.optimization_barrier(
                (weight_change, weight_before, weight_low)
            )
        else:
            weight_change = second_change(
                weight_anchor,
                weight_change.astype(jnp.float32),
                weight_before.astype(jnp.float32),
                weight_grad,
                decay_rate,
            )
            gain_change = second_change(gain_first, gain_first - gain, gain_before, gain_grad, 0.0)

    sent = with_gain(
        weight_change.astype(jnp.bfloat16).reshape(islands, owned, wide),
        gain_change[:wide].astype(jnp.bfloat16).reshape(islands, share),
    )
    arrived = lax.all_to_all(sent, ISLAND, split_axis=0, concat_axis=0, tiled=True)
    pseudo = arrived.astype(jnp.float32).sum(axis=0) / islands
    weight_pseudo, gain_pseudo = pseudo[:owned], pseudo[owned, :share]
    weight_velocity = outer_momentum * weight_moment + weight_pseudo
    gain_velocity = outer_momentum * gain_moment + gain_pseudo
    weight_updated = weight_master - outer_rate * (weight_pseudo + outer_momentum * weight_velocity)
    gain_updated = gain_master - outer_rate * (gain_pseudo + outer_momentum * gain_velocity)
    return (weight_updated, gain_updated, weight_velocity, gain_velocity)


def solution(mesh):
    torus = Mesh(mesh.devices.reshape(2, 4, 4, 2, 2), (*ISLAND, *SHARD))
    return jax.shard_map(
        per_device,
        mesh=torus,
        in_specs=(
            P(ISLAND, SHARD),
            P(SHARD_ISLAND),
            P(ISLAND, SHARD),
            P(SHARD_ISLAND),
            P(ISLAND, None, SHARD, None),
            P(ISLAND, None, None, SHARD),
            P(ISLAND, None, None, SHARD),
        ),
        out_specs=(P(ISLAND, SHARD), P(SHARD_ISLAND), P(ISLAND, SHARD), P(SHARD_ISLAND)),
        check_vma=False,
    )
```

```python
import jax
import jax.numpy as jnp
from jax import lax
from jax.experimental import pallas as pl
from jax.experimental.pallas import tpu as pltpu
from jax.sharding import Mesh
from jax.sharding import PartitionSpec as P


D = 4096
STEPS = 2
SHARD = ("y", "xh", "c")
ISLAND = ("xl", "z")
SHARD_ISLAND = ("y", "xh", "c", "xl", "z")


norm_epsilon = 1e-05
inner_rate = 0.05
beta_one = 0.9
beta_two = 0.95
adam_epsilon = 0.3
decay_rate = 0.1
outer_rate = 0.7
outer_momentum = 0.9


def core_swap(value):
    return lax.ppermute(value, "c", [(0, 1), (1, 0)])


def x_swap(value):
    return lax.ppermute(value, "xh", [(0, 1), (1, 0)])


def y_hop(value, way):
    pairs = []
    for y in range(4):
        for c in range(2):
            to = (y + (way if c == 0 else -way)) % 4
            pairs.append((y * 2 + c, to * 2 + c))
    return lax.ppermute(value, ("y", "c"), pairs)


def copy_for_each(value, axis):
    copies = jnp.broadcast_to(value, (lax.axis_size(axis), *value.shape))
    return lax.all_to_all(copies, axis, split_axis=0, concat_axis=0, tiled=True)


def gathered_pieces(own):
    a = y_hop(own, 1)
    b = y_hop(own, -1)
    x = x_swap(own)
    a2 = y_hop(x, 1)
    b2 = y_hop(x, -1)
    f = y_hop(a, 1)
    f2 = y_hop(b2, -1)
    return (own, x, a, b, a2, b2, f, f2)


BLOCK = 96
VMEM_LIMIT = 40 * 1024 * 1024


LETTERS = "oxabcefg"


def forward_kernel(letters, pieces, weight, weight_other, flow, residual_out, rows_out, rows, weights, held, made, came, loaded, streamed, left, sent):
    y, xh, c = lax.axis_index("y"), lax.axis_index("xh"), lax.axis_index("c")
    d = 1 - 2 * c
    before, after, across = (y + 4 - d) % 4, (y + 4 + d) % 4, (y + 2) % 4
    blocks = (
        (y, xh), (y, 1 - xh), (before, xh), (after, xh),
        (before, 1 - xh), (after, 1 - xh), (across, xh), (across, 1 - xh),
    )
    places = []
    for letter in letters:
        py, px = blocks[LETTERS.index(letter)]
        places.append(pl.ds(pl.multiple_of((py * 2 + px) * BLOCK, BLOCK), BLOCK))
    own = [pl.ds(at * BLOCK, BLOCK) for at in range(len(letters))]
    owned, wide = D // 8, flow.shape[1] // 2

    loads = [
        pltpu.make_async_copy(
            source.at[:, pl.ds(0, owned)], weights.at[half], loaded.at[half]
        )
        for half, source in enumerate((weight, weight_other))
    ]
    flows = [
        pltpu.make_async_copy(flow.at[to], held.at[at], streamed.at[i])
        for i, (at, to) in enumerate(zip(own, places))
    ]
    takes = [
        pltpu.make_async_copy(source, rows.at[at], came.at[i])
        for i, (at, source) in enumerate(zip(own, pieces))
    ]
    gives = [
        pltpu.make_async_copy(rows.at[at], rows_out.at[to], left.at[i])
        for i, (at, to) in enumerate(zip(own, places))
    ]
    sends = [
        pltpu.make_async_copy(made.at[at], residual_out.at[to], sent.at[i])
        for i, (at, to) in enumerate(zip(own, places))
    ]
    for copy in (loads[0], *takes[:4], *flows[:4], loads[1], *takes[4:], *flows[4:]):
        copy.start()
    for group in range(2):
        members = range(group * 4, group * 4 + 4)
        these = pl.ds(group * 4 * BLOCK, 4 * BLOCK)
        for i in members:
            takes[i].wait()
            gives[i].start()
        for i in members:
            flows[i].wait()
        for half in range(2):
            if group == 0:
                loads[half].wait()
            projected = jnp.dot(
                rows[these, :],
                weights[half].reshape(D, wide),
                preferred_element_type=jnp.float32,
            )
            columns = slice(half * wide, (half + 1) * wide)
            made[these, columns] = (
                held[these, columns].astype(jnp.float32) + projected * D ** (-0.5)
            )
        for i in members:
            sends[i].start()
    for copy in (*gives, *sends):
        copy.wait()


def forward(letters, pieces, weight, weight_other, flow, earlier=()):
    anywhere = pl.BlockSpec(memory_space=pl.ANY)
    count = len(letters)
    tokens, features = flow.shape

    def kernel(*refs):
        rest = refs[count : count + 3] + refs[count + 3 + len(earlier) :]
        forward_kernel(letters, refs[:count], *rest)

    return pl.pallas_call(
        kernel,
        out_shape=(
            jax.ShapeDtypeStruct((tokens, features), jnp.float32),
            jax.ShapeDtypeStruct((tokens, D), jnp.bfloat16),
        ),
        in_specs=[anywhere] * (count + 3 + len(earlier)),
        out_specs=(anywhere, anywhere),
        scratch_shapes=[
            pltpu.VMEM((count * BLOCK, D), jnp.bfloat16),
            pltpu.VMEM((2, 8, D // 8, features // 2), jnp.bfloat16),
            pltpu.VMEM((count * BLOCK, features), jnp.bfloat16),
            pltpu.VMEM((count * BLOCK, features), jnp.float32),
            pltpu.SemaphoreType.DMA((count,)),
            pltpu.SemaphoreType.DMA((2,)),
            pltpu.SemaphoreType.DMA((count,)),
            pltpu.SemaphoreType.DMA((count,)),
            pltpu.SemaphoreType.DMA((count,)),
        ],
        input_output_aliases={count + 3 + i: i for i in range(len(earlier))},
        compiler_params=pltpu.CompilerParams(vmem_limit_bytes=VMEM_LIMIT),
        cost_estimate=pl.CostEstimate(
            flops=2 * count * BLOCK * D * features,
            bytes_accessed=4 * count * BLOCK * D + 2 * D * features,
            transcendentals=0,
        ),
        name="forward",
    )(*pieces, weight, weight_other, flow, *earlier)


def first_update(param, gradient, decay):
    return param - inner_rate * (gradient / (jnp.abs(gradient) + adam_epsilon) + decay * param)


def second_change(anchor, change, before, gradient, decay):
    beside = (1.0 - beta_one) / (1.0 - beta_one**2)
    first_hat = (beta_one * beside) * before + beside * gradient
    beside = (1.0 - beta_two) / (1.0 - beta_two**2)
    second_hat = (beta_two * beside) * (before * before) + beside * (gradient * gradient)
    root = second_hat * lax.rsqrt(jnp.maximum(second_hat, 1e-37))
    param = anchor - change
    return change + inner_rate * (first_hat / (root + adam_epsilon) + decay * param)


def per_device(weight_master, gain_master, weight_moment, gain_moment, attended, stream, targets):
    islands = lax.axis_size(ISLAND)
    width_scale = D ** (-0.5)
    c = lax.axis_index("c")
    wide = weight_master.shape[1]

    pieces = [gathered_pieces(attended[0][step]) for step in range(STEPS)]

    def with_gain(weight_rows, gain_rows):
        filled = [(0, 0)] * (gain_rows.ndim - 1) + [(0, 15), (0, wide - gain_rows.shape[-1])]
        return jnp.concatenate([weight_rows, jnp.pad(gain_rows[..., None, :], filled)], axis=-2)

    owned, share = weight_master.shape[0], gain_master.shape[0]
    packed = with_gain(weight_master.astype(jnp.bfloat16), gain_master.astype(jnp.bfloat16))
    packed = copy_for_each(packed, ISLAND)
    packed_other = core_swap(packed)
    anchor_low = packed[:, :owned].reshape(D, wide)
    gain_anchor = packed[:, owned, :share].reshape(wide).astype(jnp.float32)
    gain_other = packed_other[:, owned, :share].reshape(wide).astype(jnp.float32)

    def token_half(value):
        blocks = value[0].reshape(STEPS, 8, 2, 96, wide)
        mine = lax.dynamic_index_in_dim(blocks, c, axis=2, keepdims=False)
        theirs = lax.dynamic_index_in_dim(blocks, 1 - c, axis=2, keepdims=False)
        both = jnp.concatenate([mine, core_swap(theirs)], axis=-1)
        return both.reshape(STEPS, 768, 2 * wide)

    stream_half = token_half(stream)
    target_half = token_half(targets)

    weight_anchor = anchor_low.astype(jnp.float32)
    gain = jnp.concatenate([gain_anchor, gain_other])
    for step in range(STEPS):
        if step == 0:
            held, held_other = packed, packed_other
        else:
            held = weight_low.reshape(islands, owned, wide)
            held_other = core_swap(held)
        residual, rows = forward(LETTERS, pieces[step], held, held_other, stream_half[step])
        goal = target_half[step].astype(jnp.float32)
        scaled = residual * gain
        sums = [
            jnp.sum(residual * residual, axis=1),
            jnp.sum(scaled * scaled, axis=1),
            jnp.sum(goal * scaled, axis=1),
        ]
        sums = jnp.concatenate(sums).reshape(1, -1)
        totals = copy_for_each(sums, ("y", "xh"))
        totals = jnp.sum(totals, axis=0).reshape(3, -1)
        inverse = lax.rsqrt(totals[0] / D + norm_epsilon)
        slope = (inverse * totals[1] - totals[2])[:, None]
        inverse = inverse[:, None]
        normed = residual * inverse * gain
        loss_grad = lax.optimization_barrier((normed - goal).astype(jnp.bfloat16))
        loss_grad = loss_grad.astype(jnp.float32)
        residual_grad = (
            inverse * (loss_grad * gain) - residual * inverse * inverse * inverse * slope / D
        ).astype(jnp.bfloat16)
        gain_grad = jnp.sum(loss_grad * residual * inverse, axis=0)

        def over_tokens(columns):
            return jnp.einsum(
                "td,tf->df", rows, residual_grad[:, columns], preferred_element_type=jnp.float32
            )

        other = over_tokens(slice(wide, None)).astype(jnp.bfloat16)
        other = core_swap(other)
        mine = lax.optimization_barrier(over_tokens(slice(0, wide)).astype(jnp.bfloat16))
        weight_grad = (mine.astype(jnp.float32) + other.astype(jnp.float32)) * width_scale
        gain_other = core_swap(gain_grad)
        gain_grad = gain_grad + jnp.concatenate([gain_other[wide:], gain_other[:wide]])
        if step == 0:
            weight_low = first_update(weight_anchor, weight_grad, decay_rate)
            weight_change = (weight_anchor - weight_low).astype(jnp.bfloat16)
            weight_before = weight_grad.astype(jnp.bfloat16)
            weight_low = weight_low.astype(jnp.bfloat16)
            gain_first = gain
            gain_before, gain = gain_grad, first_update(gain, gain_grad, 0.0)
            weight_change, weight_before, weight_low = lax.optimization_barrier(
                (weight_change, weight_before, weight_low)
            )
        else:
            weight_change = second_change(
                weight_anchor,
                weight_change.astype(jnp.float32),
                weight_before.astype(jnp.float32),
                weight_grad,
                decay_rate,
            )
            gain_change = second_change(gain_first, gain_first - gain, gain_before, gain_grad, 0.0)

    sent = with_gain(
        weight_change.astype(jnp.bfloat16).reshape(islands, owned, wide),
        gain_change[:wide].astype(jnp.bfloat16).reshape(islands, share),
    )
    arrived = lax.all_to_all(sent, ISLAND, split_axis=0, concat_axis=0, tiled=True)
    pseudo = arrived.astype(jnp.float32).sum(axis=0) / islands
    weight_pseudo, gain_pseudo = pseudo[:owned], pseudo[owned, :share]
    weight_velocity = outer_momentum * weight_moment + weight_pseudo
    gain_velocity = outer_momentum * gain_moment + gain_pseudo
    weight_updated = weight_master - outer_rate * (weight_pseudo + outer_momentum * weight_velocity)
    gain_updated = gain_master - outer_rate * (gain_pseudo + outer_momentum * gain_velocity)
    return (weight_updated, gain_updated, weight_velocity, gain_velocity)


def solution(mesh):
    torus = Mesh(mesh.devices.reshape(2, 4, 4, 2, 2), (*ISLAND, *SHARD))
    return jax.shard_map(
        per_device,
        mesh=torus,
        in_specs=(
            P(ISLAND, SHARD),
            P(SHARD_ISLAND),
            P(ISLAND, SHARD),
            P(SHARD_ISLAND),
            P(ISLAND, None, SHARD, None),
            P(ISLAND, None, None, SHARD),
            P(ISLAND, None, None, SHARD),
        ),
        out_specs=(P(ISLAND, SHARD), P(SHARD_ISLAND), P(ISLAND, SHARD), P(SHARD_ISLAND)),
        check_vma=False,
    )
```

```python
import jax
import jax.numpy as jnp
from jax import lax
from jax.experimental import pallas as pl
from jax.experimental.pallas import tpu as pltpu
from jax.sharding import Mesh
from jax.sharding import PartitionSpec as P


D = 4096
STEPS = 2
SHARD = ("y", "xh", "c")
ISLAND = ("xl", "z")
SHARD_ISLAND = ("y", "xh", "c", "xl", "z")


norm_epsilon = 1e-05
inner_rate = 0.05
beta_one = 0.9
beta_two = 0.95
adam_epsilon = 0.3
decay_rate = 0.1
outer_rate = 0.7
outer_momentum = 0.9


def core_swap(value):
    return lax.ppermute(value, "c", [(0, 1), (1, 0)])


def x_swap(value):
    return lax.ppermute(value, "xh", [(0, 1), (1, 0)])


def y_hop(value, way):
    pairs = []
    for y in range(4):
        for c in range(2):
            to = (y + (way if c == 0 else -way)) % 4
            pairs.append((y * 2 + c, to * 2 + c))
    return lax.ppermute(value, ("y", "c"), pairs)


def copy_for_each(value, axis):
    copies = jnp.broadcast_to(value, (lax.axis_size(axis), *value.shape))
    return lax.all_to_all(copies, axis, split_axis=0, concat_axis=0, tiled=True)


def gathered_pieces(own):
    a = y_hop(own, 1)
    b = y_hop(own, -1)
    x = x_swap(own)
    a2 = y_hop(x, 1)
    b2 = y_hop(x, -1)
    f = y_hop(a, 1)
    f2 = y_hop(b2, -1)
    return (own, x, a, b, a2, b2, f, f2)


BLOCK = 96
VMEM_LIMIT = 40 * 1024 * 1024


def forward_kernel(*refs):
    pieces, (weight, weight_other, flow, residual, rows_out, rows, weights, came, loaded, left) = (
        refs[:8],
        refs[8:],
    )
    y, xh, c = lax.axis_index("y"), lax.axis_index("xh"), lax.axis_index("c")
    d = 1 - 2 * c
    before, after, across = (y + 4 - d) % 4, (y + 4 + d) % 4, (y + 2) % 4
    places = [
        (py * 2 + px) * BLOCK
        for py, px in (
            (y, xh), (y, 1 - xh), (before, xh), (after, xh),
            (before, 1 - xh), (after, 1 - xh), (across, xh), (across, 1 - xh),
        )
    ]
    wide = weight.shape[2]
    loads = [
        pltpu.make_async_copy(
            source.at[:, pl.ds(0, weights.shape[2])], weights.at[half], loaded.at[half]
        )
        for half, source in enumerate((weight, weight_other))
    ]
    takes = [
        pltpu.make_async_copy(source, rows.at[pl.ds(at * BLOCK, BLOCK)], came.at[at])
        for at, source in enumerate(pieces)
    ]
    gives = [
        pltpu.make_async_copy(
            rows.at[pl.ds(at * BLOCK, BLOCK)],
            rows_out.at[pl.ds(pl.multiple_of(places[at], BLOCK), BLOCK)],
            left.at[at],
        )
        for at in range(8)
    ]
    loads[0].start()
    for take in takes[:4]:
        take.start()
    loads[1].start()
    for take in takes[4:]:
        take.start()
    for group in range(2):
        members = range(group * 4, group * 4 + 4)
        for at in members:
            takes[at].wait()
            gives[at].start()
        for half in range(2):
            if group == 0:
                loads[half].wait()
            projected = jnp.dot(
                rows[group * 4 * BLOCK : (group + 1) * 4 * BLOCK, :],
                weights[half].reshape(D, wide),
                preferred_element_type=jnp.float32,
            )
            columns = slice(half * wide, (half + 1) * wide)
            for place, at in enumerate(members):
                to = pl.ds(pl.multiple_of(places[at], BLOCK), BLOCK)
                residual[to, columns] = (
                    flow[to, columns].astype(jnp.float32)
                    + projected[place * BLOCK : (place + 1) * BLOCK] * D ** (-0.5)
                )
    for give in gives:
        give.wait()


def forward(pieces, weight, weight_other, flow):
    anywhere = pl.BlockSpec(memory_space=pl.ANY)
    inside = pl.BlockSpec(memory_space=pltpu.VMEM)
    tokens, features = flow.shape
    depth = D
    islands, _, wide = weight.shape
    return pl.pallas_call(
        forward_kernel,
        out_shape=(
            jax.ShapeDtypeStruct((tokens, features), jnp.float32),
            jax.ShapeDtypeStruct((tokens, depth), jnp.bfloat16),
        ),
        in_specs=[anywhere] * 10 + [inside],
        out_specs=(inside, pl.BlockSpec(memory_space=pltpu.HBM)),
        scratch_shapes=[
            pltpu.VMEM((tokens, depth), jnp.bfloat16),
            pltpu.VMEM((2, islands, depth // islands, wide), jnp.bfloat16),
            pltpu.SemaphoreType.DMA((8,)),
            pltpu.SemaphoreType.DMA((2,)),
            pltpu.SemaphoreType.DMA((8,)),
        ],
        compiler_params=pltpu.CompilerParams(vmem_limit_bytes=VMEM_LIMIT),
        cost_estimate=pl.CostEstimate(
            flops=2 * tokens * depth * features,
            bytes_accessed=4 * tokens * depth + 2 * depth * features,
            transcendentals=0,
        ),
        name="forward",
    )(*pieces, weight, weight_other, flow)


def first_update(param, gradient, decay):
    return param - inner_rate * (gradient / (jnp.abs(gradient) + adam_epsilon) + decay * param)


def second_change(anchor, change, before, gradient, decay):
    beside = (1.0 - beta_one) / (1.0 - beta_one**2)
    first_hat = (beta_one * beside) * before + beside * gradient
    beside = (1.0 - beta_two) / (1.0 - beta_two**2)
    second_hat = (beta_two * beside) * (before * before) + beside * (gradient * gradient)
    root = second_hat * lax.rsqrt(jnp.maximum(second_hat, 1e-37))
    param = anchor - change
    return change + inner_rate * (first_hat / (root + adam_epsilon) + decay * param)


def per_device(weight_master, gain_master, weight_moment, gain_moment, attended, stream, targets):
    islands = lax.axis_size(ISLAND)
    width_scale = D ** (-0.5)
    c = lax.axis_index("c")
    wide = weight_master.shape[1]

    pieces = [gathered_pieces(attended[0][step]) for step in range(STEPS)]

    def with_gain(weight_rows, gain_rows):
        filled = [(0, 0)] * (gain_rows.ndim - 1) + [(0, 15), (0, wide - gain_rows.shape[-1])]
        return jnp.concatenate([weight_rows, jnp.pad(gain_rows[..., None, :], filled)], axis=-2)

    owned, share = weight_master.shape[0], gain_master.shape[0]
    packed = with_gain(weight_master.astype(jnp.bfloat16), gain_master.astype(jnp.bfloat16))
    packed = copy_for_each(packed, ISLAND)
    packed_other = core_swap(packed)
    anchor_low = packed[:, :owned].reshape(D, wide)
    gain_anchor = packed[:, owned, :share].reshape(wide).astype(jnp.float32)
    gain_other = packed_other[:, owned, :share].reshape(wide).astype(jnp.float32)

    def token_half(value):
        blocks = value[0].reshape(STEPS, 8, 2, 96, wide)
        mine = lax.dynamic_index_in_dim(blocks, c, axis=2, keepdims=False)
        theirs = lax.dynamic_index_in_dim(blocks, 1 - c, axis=2, keepdims=False)
        both = jnp.concatenate([mine, core_swap(theirs)], axis=-1)
        return both.reshape(STEPS, 768, 2 * wide)

    stream_half = token_half(stream)
    target_half = token_half(targets)

    weight_anchor = anchor_low.astype(jnp.float32)
    gain = jnp.concatenate([gain_anchor, gain_other])
    for step in range(STEPS):
        if step == 0:
            held, held_other = packed, packed_other
        else:
            held = weight_low.reshape(islands, owned, wide)
            held_other = core_swap(held)
        residual, rows = forward(pieces[step], held, held_other, stream_half[step])
        goal = target_half[step].astype(jnp.float32)
        scaled = residual * gain
        sums = [
            jnp.sum(residual * residual, axis=1),
            jnp.sum(scaled * scaled, axis=1),
            jnp.sum(goal * scaled, axis=1),
        ]
        sums = jnp.concatenate(sums).reshape(1, -1)
        totals = copy_for_each(sums, ("y", "xh"))
        totals = jnp.sum(totals, axis=0).reshape(3, -1)
        inverse = lax.rsqrt(totals[0] / D + norm_epsilon)
        slope = (inverse * totals[1] - totals[2])[:, None]
        inverse = inverse[:, None]
        normed = residual * inverse * gain
        loss_grad = lax.optimization_barrier((normed - goal).astype(jnp.bfloat16))
        loss_grad = loss_grad.astype(jnp.float32)
        residual_grad = (
            inverse * (loss_grad * gain) - residual * inverse * inverse * inverse * slope / D
        ).astype(jnp.bfloat16)
        gain_grad = jnp.sum(loss_grad * residual * inverse, axis=0)

        def over_tokens(columns):
            return jnp.einsum(
                "td,tf->df", rows, residual_grad[:, columns], preferred_element_type=jnp.float32
            )

        other = over_tokens(slice(wide, None)).astype(jnp.bfloat16)
        other = core_swap(other)
        mine = lax.optimization_barrier(over_tokens(slice(0, wide)).astype(jnp.bfloat16))
        weight_grad = (mine.astype(jnp.float32) + other.astype(jnp.float32)) * width_scale
        gain_other = core_swap(gain_grad)
        gain_grad = gain_grad + jnp.concatenate([gain_other[wide:], gain_other[:wide]])
        if step == 0:
            weight_low = first_update(weight_anchor, weight_grad, decay_rate)
            weight_change = (weight_anchor - weight_low).astype(jnp.bfloat16)
            weight_before = weight_grad.astype(jnp.bfloat16)
            weight_low = weight_low.astype(jnp.bfloat16)
            gain_first = gain
            gain_before, gain = gain_grad, first_update(gain, gain_grad, 0.0)
            weight_change, weight_before, weight_low = lax.optimization_barrier(
                (weight_change, weight_before, weight_low)
            )
        else:
            weight_change = second_change(
                weight_anchor,
                weight_change.astype(jnp.float32),
                weight_before.astype(jnp.float32),
                weight_grad,
                decay_rate,
            )
            gain_change = second_change(gain_first, gain_first - gain, gain_before, gain_grad, 0.0)

    sent = with_gain(
        weight_change.astype(jnp.bfloat16).reshape(islands, owned, wide),
        gain_change[:wide].astype(jnp.bfloat16).reshape(islands, share),
    )
    arrived = lax.all_to_all(sent, ISLAND, split_axis=0, concat_axis=0, tiled=True)
    pseudo = arrived.astype(jnp.float32).sum(axis=0) / islands
    weight_pseudo, gain_pseudo = pseudo[:owned], pseudo[owned, :share]
    weight_velocity = outer_momentum * weight_moment + weight_pseudo
    gain_velocity = outer_momentum * gain_moment + gain_pseudo
    weight_updated = weight_master - outer_rate * (weight_pseudo + outer_momentum * weight_velocity)
    gain_updated = gain_master - outer_rate * (gain_pseudo + outer_momentum * gain_velocity)
    return (weight_updated, gain_updated, weight_velocity, gain_velocity)


def solution(mesh):
    torus = Mesh(mesh.devices.reshape(2, 4, 4, 2, 2), (*ISLAND, *SHARD))
    return jax.shard_map(
        per_device,
        mesh=torus,
        in_specs=(
            P(ISLAND, SHARD),
            P(SHARD_ISLAND),
            P(ISLAND, SHARD),
            P(SHARD_ISLAND),
            P(ISLAND, None, SHARD, None),
            P(ISLAND, None, None, SHARD),
            P(ISLAND, None, None, SHARD),
        ),
        out_specs=(P(ISLAND, SHARD), P(SHARD_ISLAND), P(ISLAND, SHARD), P(SHARD_ISLAND)),
        check_vma=False,
    )
```

```python
import jax
import jax.numpy as jnp
from jax import lax
from jax.experimental import pallas as pl
from jax.experimental.pallas import tpu as pltpu
from jax.sharding import Mesh
from jax.sharding import PartitionSpec as P


D = 4096
STEPS = 2
SHARD = ("y", "xh", "c")
ISLAND = ("xl", "z")
SHARD_ISLAND = ("y", "xh", "c", "xl", "z")


norm_epsilon = 1e-05
inner_rate = 0.05
beta_one = 0.9
beta_two = 0.95
adam_epsilon = 0.3
decay_rate = 0.1
outer_rate = 0.7
outer_momentum = 0.9


def core_swap(value):
    return lax.ppermute(value, "c", [(0, 1), (1, 0)])


def x_swap(value):
    return lax.ppermute(value, "xh", [(0, 1), (1, 0)])


def y_hop(value, way):
    pairs = []
    for y in range(4):
        for c in range(2):
            to = (y + (way if c == 0 else -way)) % 4
            pairs.append((y * 2 + c, to * 2 + c))
    return lax.ppermute(value, ("y", "c"), pairs)


def copy_for_each(value, axis):
    copies = jnp.broadcast_to(value, (lax.axis_size(axis), *value.shape))
    return lax.all_to_all(copies, axis, split_axis=0, concat_axis=0, tiled=True)


def gathered_pieces(own):
    a = y_hop(own, 1)
    b = y_hop(own, -1)
    x = x_swap(own)
    a2 = y_hop(x, 1)
    b2 = y_hop(x, -1)
    f = y_hop(a, 1)
    f2 = y_hop(b2, -1)
    return (own, x, a, b, a2, b2, f, f2)


BLOCK = 96
VMEM_LIMITS = (40, 40)


def forward_kernel(*refs):
    pieces, (weight, weight_other, flow, residual, rows_out, rows, weights, came, loaded, left) = (
        refs[:8],
        refs[8:],
    )
    y, xh, c = lax.axis_index("y"), lax.axis_index("xh"), lax.axis_index("c")
    d = 1 - 2 * c
    before, after, across = (y + 4 - d) % 4, (y + 4 + d) % 4, (y + 2) % 4
    places = [
        (py * 2 + px) * BLOCK
        for py, px in (
            (y, xh), (y, 1 - xh), (before, xh), (after, xh),
            (before, 1 - xh), (after, 1 - xh), (across, xh), (across, 1 - xh),
        )
    ]
    wide = weight.shape[2]
    loads = [
        pltpu.make_async_copy(
            source.at[:, pl.ds(0, weights.shape[2])], weights.at[half], loaded.at[half]
        )
        for half, source in enumerate((weight, weight_other))
    ]
    takes = [
        pltpu.make_async_copy(source, rows.at[pl.ds(at * BLOCK, BLOCK)], came.at[at])
        for at, source in enumerate(pieces)
    ]
    gives = [
        pltpu.make_async_copy(
            rows.at[pl.ds(at * BLOCK, BLOCK)],
            rows_out.at[pl.ds(pl.multiple_of(places[at], BLOCK), BLOCK)],
            left.at[at],
        )
        for at in range(8)
    ]
    loads[0].start()
    for take in takes[:4]:
        take.start()
    loads[1].start()
    for take in takes[4:]:
        take.start()
    for group in range(2):
        members = range(group * 4, group * 4 + 4)
        for at in members:
            takes[at].wait()
            gives[at].start()
        for half in range(2):
            if group == 0:
                loads[half].wait()
            projected = jnp.dot(
                rows[group * 4 * BLOCK : (group + 1) * 4 * BLOCK, :],
                weights[half].reshape(D, wide),
                preferred_element_type=jnp.float32,
            )
            columns = slice(half * wide, (half + 1) * wide)
            for place, at in enumerate(members):
                to = pl.ds(pl.multiple_of(places[at], BLOCK), BLOCK)
                residual[to, columns] = (
                    flow[to, columns].astype(jnp.float32)
                    + projected[place * BLOCK : (place + 1) * BLOCK] * D ** (-0.5)
                )
    for give in gives:
        give.wait()


def forward(pieces, weight, weight_other, flow, vmem_limit):
    anywhere = pl.BlockSpec(memory_space=pl.ANY)
    inside = pl.BlockSpec(memory_space=pltpu.VMEM)
    tokens, features = flow.shape
    depth = D
    islands, _, wide = weight.shape
    return pl.pallas_call(
        forward_kernel,
        out_shape=(
            jax.ShapeDtypeStruct((tokens, features), jnp.float32),
            jax.ShapeDtypeStruct((tokens, depth), jnp.bfloat16),
        ),
        in_specs=[anywhere] * 10 + [inside],
        out_specs=(inside, pl.BlockSpec(memory_space=pltpu.HBM)),
        scratch_shapes=[
            pltpu.VMEM((tokens, depth), jnp.bfloat16),
            pltpu.VMEM((2, islands, depth // islands, wide), jnp.bfloat16),
            pltpu.SemaphoreType.DMA((8,)),
            pltpu.SemaphoreType.DMA((2,)),
            pltpu.SemaphoreType.DMA((8,)),
        ],
        compiler_params=pltpu.CompilerParams(vmem_limit_bytes=vmem_limit * 1024 * 1024),
        cost_estimate=pl.CostEstimate(
            flops=2 * tokens * depth * features,
            bytes_accessed=4 * tokens * depth + 2 * depth * features,
            transcendentals=0,
        ),
        name="forward",
    )(*pieces, weight, weight_other, flow)


def first_update(param, gradient, decay):
    return param - inner_rate * (gradient / (jnp.abs(gradient) + adam_epsilon) + decay * param)


def second_change(anchor, change, before, gradient, decay):
    beside = (1.0 - beta_one) / (1.0 - beta_one**2)
    first_hat = (beta_one * beside) * before + beside * gradient
    beside = (1.0 - beta_two) / (1.0 - beta_two**2)
    second_hat = (beta_two * beside) * (before * before) + beside * (gradient * gradient)
    root = second_hat * lax.rsqrt(jnp.maximum(second_hat, 1e-37))
    param = anchor - change
    return change + inner_rate * (first_hat / (root + adam_epsilon) + decay * param)


def per_device(weight_master, gain_master, weight_moment, gain_moment, attended, stream, targets):
    islands = lax.axis_size(ISLAND)
    width_scale = D ** (-0.5)
    c = lax.axis_index("c")
    wide = weight_master.shape[1]

    pieces = [gathered_pieces(attended[0][0])]
    later, _ = lax.optimization_barrier((attended, pieces[0][2]))
    pieces.append(gathered_pieces(later[0][1]))

    def with_gain(weight_rows, gain_rows):
        filled = [(0, 0)] * (gain_rows.ndim - 1) + [(0, 15), (0, wide - gain_rows.shape[-1])]
        return jnp.concatenate([weight_rows, jnp.pad(gain_rows[..., None, :], filled)], axis=-2)

    owned, share = weight_master.shape[0], gain_master.shape[0]
    packed = with_gain(weight_master.astype(jnp.bfloat16), gain_master.astype(jnp.bfloat16))
    packed = copy_for_each(packed, ISLAND)
    packed_other = core_swap(packed)
    anchor_low = packed[:, :owned].reshape(D, wide)
    gain_anchor = packed[:, owned, :share].reshape(wide).astype(jnp.float32)
    gain_other = packed_other[:, owned, :share].reshape(wide).astype(jnp.float32)

    def token_half(value):
        blocks = value[0].reshape(STEPS, 8, 2, 96, wide)
        mine = lax.dynamic_index_in_dim(blocks, c, axis=2, keepdims=False)
        theirs = lax.dynamic_index_in_dim(blocks, 1 - c, axis=2, keepdims=False)
        both = jnp.concatenate([mine, core_swap(theirs)], axis=-1)
        return both.reshape(STEPS, 768, 2 * wide)

    stream_half = token_half(stream)
    target_half = token_half(targets)

    weight_anchor = anchor_low.astype(jnp.float32)
    gain = jnp.concatenate([gain_anchor, gain_other])
    for step in range(STEPS):
        if step == 0:
            held, held_other = packed, packed_other
        else:
            held = weight_low.reshape(islands, owned, wide)
            held_other = core_swap(held)
        residual, rows = forward(
            pieces[step], held, held_other, stream_half[step], VMEM_LIMITS[step]
        )
        goal = target_half[step].astype(jnp.float32)
        scaled = residual * gain
        sums = [
            jnp.sum(residual * residual, axis=1),
            jnp.sum(scaled * scaled, axis=1),
            jnp.sum(goal * scaled, axis=1),
        ]
        sums = jnp.concatenate(sums).reshape(1, -1)
        totals = copy_for_each(sums, ("y", "xh"))
        totals = jnp.sum(totals, axis=0).reshape(3, -1)
        inverse = lax.rsqrt(totals[0] / D + norm_epsilon)
        slope = (inverse * totals[1] - totals[2])[:, None]
        inverse = inverse[:, None]
        normed = residual * inverse * gain
        loss_grad = lax.optimization_barrier((normed - goal).astype(jnp.bfloat16))
        loss_grad = loss_grad.astype(jnp.float32)
        residual_grad = (
            inverse * (loss_grad * gain) - residual * inverse * inverse * inverse * slope / D
        ).astype(jnp.bfloat16)
        gain_grad = jnp.sum(loss_grad * residual * inverse, axis=0)

        def over_tokens(columns):
            return jnp.einsum(
                "td,tf->df", rows, residual_grad[:, columns], preferred_element_type=jnp.float32
            )

        other = over_tokens(slice(wide, None)).astype(jnp.bfloat16)
        other = core_swap(other)
        mine = lax.optimization_barrier(over_tokens(slice(0, wide)).astype(jnp.bfloat16))
        weight_grad = (mine.astype(jnp.float32) + other.astype(jnp.float32)) * width_scale
        gain_other = core_swap(gain_grad)
        gain_grad = gain_grad + jnp.concatenate([gain_other[wide:], gain_other[:wide]])
        if step == 0:
            weight_low = first_update(weight_anchor, weight_grad, decay_rate)
            weight_change = (weight_anchor - weight_low).astype(jnp.bfloat16)
            weight_before = weight_grad.astype(jnp.bfloat16)
            weight_low = weight_low.astype(jnp.bfloat16)
            gain_first = gain
            gain_before, gain = gain_grad, first_update(gain, gain_grad, 0.0)
            weight_change, weight_before, weight_low = lax.optimization_barrier(
                (weight_change, weight_before, weight_low)
            )
        else:
            weight_change = second_change(
                weight_anchor,
                weight_change.astype(jnp.float32),
                weight_before.astype(jnp.float32),
                weight_grad,
                decay_rate,
            )
            gain_change = second_change(gain_first, gain_first - gain, gain_before, gain_grad, 0.0)

    sent = with_gain(
        weight_change.astype(jnp.bfloat16).reshape(islands, owned, wide),
        gain_change[:wide].astype(jnp.bfloat16).reshape(islands, share),
    )
    arrived = lax.all_to_all(sent, ISLAND, split_axis=0, concat_axis=0, tiled=True)
    pseudo = arrived.astype(jnp.float32).sum(axis=0) / islands
    weight_pseudo, gain_pseudo = pseudo[:owned], pseudo[owned, :share]
    weight_velocity = outer_momentum * weight_moment + weight_pseudo
    gain_velocity = outer_momentum * gain_moment + gain_pseudo
    weight_updated = weight_master - outer_rate * (weight_pseudo + outer_momentum * weight_velocity)
    gain_updated = gain_master - outer_rate * (gain_pseudo + outer_momentum * gain_velocity)
    return (weight_updated, gain_updated, weight_velocity, gain_velocity)


def solution(mesh):
    torus = Mesh(mesh.devices.reshape(2, 4, 4, 2, 2), (*ISLAND, *SHARD))
    return jax.shard_map(
        per_device,
        mesh=torus,
        in_specs=(
            P(ISLAND, SHARD),
            P(SHARD_ISLAND),
            P(ISLAND, SHARD),
            P(SHARD_ISLAND),
            P(ISLAND, None, SHARD, None),
            P(ISLAND, None, None, SHARD),
            P(ISLAND, None, None, SHARD),
        ),
        out_specs=(P(ISLAND, SHARD), P(SHARD_ISLAND), P(ISLAND, SHARD), P(SHARD_ISLAND)),
        check_vma=False,
    )
```
